32 devices in a mesh: replica: 1 (over z), data: 4 (over y), table: 8 (over x, core).
Axes of the slice: x: 4, y: 4, z: 1, core: 2. Of those that a mesh axis runs over, the one named last changes fastest.
The devices are a block of a 4x4x8 slice.
Arguments:
- tokens: bfloat16 [4096, 1024], P(('replica', 'data', 'table'))
- grad_out: bfloat16 [4096, 1024], P(('replica', 'data', 'table'))
- table_u: bfloat16 [131072, 1024], P(('replica', 'table'))
- table_v: bfloat16 [131072, 1024], P(('replica', 'table'))
- wanted_ids: int32 [32, 256], P(('replica', 'data', 'table'))
- pick_idx: int32 [4096, 4, 32], P(('replica', 'data', 'table'))
- gate_val: float32 [4096, 4, 32], P(('replica', 'data', 'table'))
Outputs:
- output 1: bfloat16 [4096, 1024], P(('replica', 'data', 'table'))
- output 2: bfloat16 [4096, 1024], P(('replica', 'data', 'table'))
- output 3: bfloat16 [131072, 1024], P(('replica', 'table'))
- output 4: bfloat16 [131072, 1024], P(('replica', 'table'))
All inputs are finite; a program needn't handle non-finite values.
Results may differ from the reference program's by a relative error of at most 0.00775731.
Values are sent between devices in bfloat16 or wider.
A program may use at most 768 MiB of HBM per device.

```python
import math
import jax
import jax.numpy as jnp
from jax import lax

D = 1024
N = 131072
HEADS = 4
TOPK = 32
TOK_DEV = 128
DATA = 4
TABLE = 8
POOL = 32

N_LOCAL = N // TABLE
DEVS = DATA * TABLE
T_PART = DEVS * TOK_DEV
SEL_TOK = HEADS * TOPK
SEL_DEV = TOK_DEV * SEL_TOK
ENTRIES = TABLE * POOL
BLOCK = math.gcd(TOK_DEV, max(1, 8192 // SEL_TOK))


def draw_routing(route_key):
    perm_key, off_key, own_key_a, own_key_b, slot_key, mix_key = jax.random.split(route_key, 6)
    orders = jax.vmap(lambda one_key: jax.random.permutation(one_key, N_LOCAL))(jax.random.split(perm_key, TABLE))
    offsets = jax.random.randint(off_key, (DEVS, TABLE, 1), 0, 2 * POOL)
    spot_idx = (offsets + jnp.arange(POOL, dtype=jnp.int32)[None, None, :]) % N_LOCAL
    owner_idx = jnp.arange(TABLE, dtype=jnp.int32)[None, :, None]
    local_rows = orders[owner_idx, spot_idx]
    wanted = (local_rows + owner_idx * N_LOCAL).reshape(DEVS, ENTRIES).astype(jnp.int32)
    extra_len = SEL_DEV - ENTRIES
    own_a = jax.random.randint(own_key_a, (DEVS, extra_len), 0, TABLE)
    own_b = jax.random.randint(own_key_b, (DEVS, extra_len), 0, TABLE)
    slot_idx = jax.random.randint(slot_key, (DEVS, extra_len), 0, POOL)
    extra_picks = jnp.minimum(own_a, own_b) * POOL + slot_idx
    cover = jnp.broadcast_to(jnp.arange(ENTRIES, dtype=jnp.int32)[None, :], (DEVS, ENTRIES))
    pick_all = jnp.concatenate([cover, extra_picks.astype(jnp.int32)], axis=1)
    shuffle = jax.vmap(lambda one_key: jax.random.permutation(one_key, SEL_DEV))(jax.random.split(mix_key, DEVS))
    pick_all = jnp.take_along_axis(pick_all, shuffle, axis=1)
    return wanted, pick_all.reshape(T_PART, HEADS, TOPK).astype(jnp.int32)


def setup_inputs(seed: int = 0, part: int = 0) -> dict:
    part_key = jax.random.fold_in(jax.random.key(seed), part)
    key_list = jax.random.split(part_key, 6)
    tokens = jax.random.normal(key_list[0], (T_PART, D), jnp.float32).astype(jnp.bfloat16)
    grad_out = jax.random.normal(key_list[1], (T_PART, D), jnp.float32).astype(jnp.bfloat16)
    table_u = (jax.random.normal(key_list[2], (N, D), jnp.float32) * D ** -0.5).astype(jnp.bfloat16)
    table_v = (jax.random.normal(key_list[3], (N, D), jnp.float32) * SEL_TOK ** -0.5).astype(jnp.bfloat16)
    wanted_ids, pick_idx = draw_routing(key_list[4])
    gate_val = jax.random.uniform(key_list[5], (T_PART, HEADS, TOPK), jnp.float32, 0.5, 1.5)
    return {'tokens': tokens, 'grad_out': grad_out, 'table_u': table_u, 'table_v': table_v, 'wanted_ids': wanted_ids, 'pick_idx': pick_idx, 'gate_val': gate_val}


def gelu_pair(pre_act):
    cdf_val = 0.5 * (1.0 + lax.erf(pre_act * 0.7071067811865476))
    pdf_val = jnp.exp(-0.5 * pre_act * pre_act) * 0.3989422804014327
    return pre_act * cdf_val, cdf_val + pre_act * pdf_val


def reference(tokens, grad_out, table_u, table_v, wanted_ids, pick_idx, gate_val):
    sel_ids = jnp.take_along_axis(wanted_ids, pick_idx.reshape(DEVS, SEL_DEV), axis=1)
    num_blocks = T_PART // BLOCK
    inputs = (tokens.reshape(num_blocks, BLOCK, D), grad_out.reshape(num_blocks, BLOCK, D), sel_ids.reshape(num_blocks, BLOCK, SEL_TOK), gate_val.reshape(num_blocks, BLOCK, SEL_TOK))

    def body(acc_pair, block_in):
        acc_u, acc_v = acc_pair
        x_blk, dy_blk, id_blk, gate_blk = block_in
        x_f = x_blk.astype(jnp.float32)
        dy_f = dy_blk.astype(jnp.float32)
        sel_u = jnp.take(table_u, id_blk, axis=0).astype(jnp.float32)
        sel_v = jnp.take(table_v, id_blk, axis=0).astype(jnp.float32)
        pre_act = jnp.einsum('bsd,bd->bs', sel_u, x_f)
        act_val, slope_val = gelu_pair(pre_act)
        weight = gate_blk * act_val
        y_blk = jnp.einsum('bs,bsd->bd', weight, sel_v)
        v_dot_dy = jnp.einsum('bsd,bd->bs', sel_v, dy_f)
        coef_sel = gate_blk * slope_val * v_dot_dy
        dx_blk = jnp.einsum('bs,bsd->bd', coef_sel, sel_u)
        flat_ids = id_blk.reshape(-1)
        acc_u = acc_u.at[flat_ids].add((coef_sel[:, :, None] * x_f[:, None, :]).reshape(-1, D))
        acc_v = acc_v.at[flat_ids].add((weight[:, :, None] * dy_f[:, None, :]).reshape(-1, D))
        return (acc_u, acc_v), (y_blk.astype(jnp.bfloat16), dx_blk.astype(jnp.bfloat16))

    zero_acc = jnp.zeros((N, D), jnp.float32)
    (acc_u, acc_v), (y_st, dx_st) = lax.scan(body, (zero_acc, zero_acc), inputs)
    return (y_st.reshape(T_PART, D), dx_st.reshape(T_PART, D), acc_u.astype(jnp.bfloat16), acc_v.astype(jnp.bfloat16))
```

```python
import functools
import jax
import jax.numpy as jnp
from jax import lax
from jax.experimental import pallas as pl
from jax.experimental.pallas import tpu as pltpu
from jax.sharding import PartitionSpec as P

F32 = jnp.float32
BF16 = jnp.bfloat16
VMEM_LIMIT = 60 * 1024 * 1024
MESH = pl.DeviceIdType.MESH
LANES = 128


def partner(index, k):
    out, bit = 0, 1
    while bit <= k or bit < 2:
        old = (index // bit) % 2
        out = out + ((1 - old) if k & bit else old) * bit
        bit *= 2
    return out + (index // bit) * bit


def visit_order(n):
    chips = max(1, n // 2)
    return sorted(range(n), key=lambda k: (max(min(abs(c - (c ^ (k // 2))), chips - abs(c - (c ^ (k // 2)))) for c in range(chips)), k))


def gelu_pair(pre_act):
    cdf_val = 0.5 * (1.0 + lax.erf(pre_act * 0.7071067811865476))
    pdf_val = jnp.exp(-0.5 * pre_act * pre_act) * 0.3989422804014327
    return pre_act * cdf_val, cdf_val + pre_act * pdf_val


def three_terms(val):
    hi = val.astype(BF16)
    rest = val - hi.astype(F32)
    mid = rest.astype(BF16)
    low = (rest - mid.astype(F32)).astype(BF16)
    return jnp.concatenate([hi, mid, low], axis=0)


def exact_dot(val, rhs):
    rows = val.shape[0]
    out = jnp.dot(three_terms(val), rhs, preferred_element_type=F32)
    return out[:rows] + out[rows:2 * rows] + out[2 * rows:]


def nt_dot(lhs, rhs):
    return lax.dot_general(lhs, rhs, (((1,), (1,)), ((), ())), preferred_element_type=F32)


def ids_kernel(table_n, pool, wanted_ref, pick_ref, gate_ref, ids_ref, gt_ref, out_buf, land, pick_t, gate_t, send_sem, recv_sem):
    me = lax.axis_index('table')
    others = range(1, table_n)
    barrier = pltpu.get_barrier_semaphore()
    for k in others:
        pl.semaphore_signal(barrier, inc=1, device_id={'table': partner(me, k)}, device_id_type=MESH)
    for e in range(table_n):
        out_buf[e, :, 0:pool] = wanted_ref[:, e * pool:(e + 1) * pool]
    land[me] = out_buf[me]
    pl.semaphore_wait(barrier, table_n - 1)
    copies = []
    for k in others:
        to = partner(me, k)
        copies.append(pltpu.make_async_remote_copy(src_ref=out_buf.at[to], dst_ref=land.at[me], send_sem=send_sem.at[k], recv_sem=recv_sem.at[k], device_id={'table': to}, device_id_type=MESH))
        copies[-1].start()

    toks, heads, topk = pick_ref.shape
    for h in range(heads):
        pick_t[h * topk:(h + 1) * topk, :] = pick_ref[:, h, :].astype(F32).T
        gate_t[h * topk:(h + 1) * topk, :] = gate_ref[:, h, :].T
    entries = gt_ref.shape[0]
    entry = lax.broadcasted_iota(jnp.int32, (entries, toks), 0).astype(F32)

    def add_gate(i, acc):
        for j in range(8):
            s = i * 8 + j
            acc = acc + jnp.where(entry == pick_t[pl.ds(s, 1), :], gate_t[pl.ds(s, 1), :], 0.0)
        return acc
    gt_ref[...] = lax.fori_loop(0, heads * topk // 8, add_gate, jnp.zeros((entries, toks), F32))
    for one in copies:
        one.wait()
    ids_ref[...] = land[...]


def share_ids(wanted, pick, gate, table_n, pool):
    toks, heads, topk = pick.shape
    vm = pl.BlockSpec(memory_space=pltpu.VMEM)
    return pl.pallas_call(
        functools.partial(ids_kernel, table_n, pool),
        out_shape=(jax.ShapeDtypeStruct((table_n, 1, LANES), jnp.int32), jax.ShapeDtypeStruct((table_n * pool, toks), F32)),
        in_specs=[vm] * 3,
        out_specs=(vm, vm),
        scratch_shapes=[
            pltpu.VMEM((table_n, 1, LANES), jnp.int32),
            pltpu.VMEM((table_n, 1, LANES), jnp.int32),
            pltpu.VMEM((heads * topk, toks), F32),
            pltpu.VMEM((heads * topk, toks), F32),
            pltpu.SemaphoreType.DMA((table_n,)),
            pltpu.SemaphoreType.DMA((table_n,)),
        ],
        compiler_params=pltpu.CompilerParams(collective_id=0, has_side_effects=True, vmem_limit_bytes=VMEM_LIMIT),
        name="share_ids",
    )(wanted, pick, gate)


def fetch_kernel(table_n, pool, n_local, ids_ref, u_ref, v_ref, rows_ref, tiles, sem):
    first = lax.axis_index('table') * n_local
    for owner in range(table_n):
        def start(i, carry, owner=owner):
            tile = lax.shift_right_logical(ids_ref[owner, 0, i] - first, 3)
            pltpu.make_async_copy(u_ref.at[tile], tiles.at[owner, 0, i], sem.at[owner]).start()
            pltpu.make_async_copy(v_ref.at[tile], tiles.at[owner, 1, i], sem.at[owner]).start()
            return carry
        lax.fori_loop(0, pool, start, 0, unroll=True)

    width = u_ref.shape[2]
    sub = lax.broadcasted_iota(jnp.int32, (8, width), 0)
    for owner in range(table_n):
        pltpu.make_async_copy(tiles.at[owner], tiles.at[owner], sem.at[owner]).wait()
        for which in range(2):
            def pull(g, carry, owner=owner, which=which):
                out = jnp.zeros((8, width), F32)
                for i in range(8):
                    k = g * 8 + i
                    line = jnp.bitwise_and(ids_ref[owner, 0, k] - first, 7)
                    turned = pltpu.roll(tiles[owner, which, k].astype(F32), jnp.bitwise_and(i - line + 8, 7), 0)
                    out = jnp.where(sub == i, turned, out)
                rows_ref[owner, which, pl.ds(pl.multiple_of(g * 8, 8), 8), :] = out.astype(BF16)
                return carry
            lax.fori_loop(0, pool // 8, pull, 0)


def fetch(ids, u_tiles, v_tiles, table_n, pool):
    width = u_tiles.shape[2]
    hbm = pl.BlockSpec(memory_space=pl.ANY)
    return pl.pallas_call(
        functools.partial(fetch_kernel, table_n, pool, u_tiles.shape[0] * 8),
        out_shape=jax.ShapeDtypeStruct((table_n, 2, pool, width), BF16),
        in_specs=[pl.BlockSpec(memory_space=pltpu.SMEM), hbm, hbm],
        out_specs=pl.BlockSpec(memory_space=pltpu.VMEM),
        scratch_shapes=[pltpu.VMEM((table_n, 2, pool, 8, width), BF16), pltpu.SemaphoreType.DMA((table_n,))],
        compiler_params=pltpu.CompilerParams(vmem_limit_bytes=VMEM_LIMIT),
        name="fetch_rows",
    )(ids, u_tiles, v_tiles)


def exchange_kernel(table_n, data_n, pool, send_ref, x_ref, dy_ref, gt_ref, ids_ref,
                    y_ref, dx_ref, own_u, own_v, prev_u, prev_v, next_u, next_v, ids_out,
                    rows_in, part, own, w_all, c_all,
                    a_send, a_recv, b_send, b_recv, c_send, c_recv, i_send, i_recv, o_sem):
    me = lax.axis_index('table')
    row = lax.axis_index('data')
    after, before, across = (row + 1) % data_n, (row + data_n - 1) % data_n, (row + 2) % data_n
    others = [k for k in visit_order(table_n) if k]
    along = (after, before, across)
    barrier = pltpu.get_barrier_semaphore()
    for k in others:
        pl.semaphore_signal(barrier, inc=1, device_id={'table': partner(me, k)}, device_id_type=MESH)
    for to in along:
        pl.semaphore_signal(barrier, inc=1, device_id={'data': to}, device_id_type=MESH)
    pl.semaphore_wait(barrier, len(others) + len(along))

    def remote(src, dst, sem_s, sem_r, **to):
        copy = pltpu.make_async_remote_copy(src_ref=src, dst_ref=dst, send_sem=sem_s, recv_sem=sem_r, device_id=to, device_id_type=MESH)
        copy.start()
        return copy

    copies_a, copies_b, copies_c, local = {}, {}, [], []
    for k in others:
        to = partner(me, k)
        copies_a[k] = remote(send_ref.at[to], rows_in.at[k], a_send.at[k], a_recv.at[k], table=to)
    for j, to in enumerate(along):
        copies_c.append(remote(ids_ref, ids_out.at[j + 1], i_send.at[j], i_recv.at[j], data=to))
    local.append(pltpu.make_async_copy(ids_ref, ids_out.at[0], o_sem.at[0]))
    local[-1].start()

    def spread_on(k):
        e = partner(me, k)
        if k:
            copies_b[k].wait_recv()
        for w, (mine, prev, nxt) in enumerate(((own_u, prev_u, next_u), (own_v, prev_v, next_v))):
            copies_c.append(remote(own.at[e, w], prev.at[e], c_send.at[k, w], c_recv.at[k, w], data=after))
            copies_c.append(remote(own.at[e, w], nxt.at[e], c_send.at[k, 2 + w], c_recv.at[k, 2 + w], data=before))
        for w, mine in enumerate((own_u, own_v)):
            local.append(pltpu.make_async_copy(own.at[e, w], mine.at[e], o_sem.at[1 + 2 * k + w]))
            local[-1].start()

    x = x_ref[...]
    dy = dy_ref[...]
    order = [0] + others
    lag = 2
    for i, k in enumerate(order):
        e = partner(me, k)
        if k:
            copies_a[k].wait_recv()
        else:
            rows_in[0] = send_ref[me]
        pre = nt_dot(rows_in[k, 0], x)
        v_dy = nt_dot(rows_in[k, 1], dy)
        act, slope = gelu_pair(pre)
        gate = gt_ref[pl.ds(pl.multiple_of(e * pool, pool), pool), :]
        weight = gate * act
        coef = gate * slope * v_dy
        w_all[k * pool:(k + 1) * pool, :] = weight
        c_all[k * pool:(k + 1) * pool, :] = coef
        part_u = exact_dot(coef, x).astype(BF16)
        part_v = exact_dot(weight, dy).astype(BF16)
        if k:
            part[k, 0] = part_u
            part[k, 1] = part_v
            copies_b[k] = remote(part.at[k], own.at[me], b_send.at[k], b_recv.at[k], table=e)
        else:
            own[me, 0] = part_u
            own[me, 1] = part_v
            spread_on(0)
        if i > lag:
            spread_on(order[i - lag])
    for k in order[-lag:]:
        spread_on(k)

    width = x_ref.shape[1]
    y_ref[...] = exact_dot(w_all[...].T, rows_in[:, 1].reshape(table_n * pool, width)).astype(BF16)
    dx_ref[...] = exact_dot(c_all[...].T, rows_in[:, 0].reshape(table_n * pool, width)).astype(BF16)

    for k in others:
        copies_a[k].wait_send()
        copies_b[k].wait_send()
    for one in copies_c:
        one.wait()
    for one in local:
        one.wait()


def exchange(rows, x, dy, gt, ids, table_n, data_n, pool):
    toks, width = x.shape
    entries = table_n * pool
    vm = pl.BlockSpec(memory_space=pltpu.VMEM)
    hbm = pl.BlockSpec(memory_space=pl.ANY)
    block = jax.ShapeDtypeStruct((table_n, pool, width), BF16)
    tok_shape = jax.ShapeDtypeStruct((toks, width), BF16)
    dma = pltpu.SemaphoreType.DMA
    return pl.pallas_call(
        functools.partial(exchange_kernel, table_n, data_n, pool),
        out_shape=(tok_shape, tok_shape) + (block,) * 6 + (jax.ShapeDtypeStruct((4, table_n, 1, LANES), jnp.int32),),
        in_specs=[vm] * 5,
        out_specs=(vm, vm) + (hbm,) * 7,
        scratch_shapes=[
            pltpu.VMEM((table_n, 2, pool, width), BF16),
            pltpu.VMEM((table_n, 2, pool, width), BF16),
            pltpu.VMEM((table_n, 2, pool, width), BF16),
            pltpu.VMEM((entries, toks), F32),
            pltpu.VMEM((entries, toks), F32),
            dma((table_n,)), dma((table_n,)), dma((table_n,)), dma((table_n,)),
            dma((table_n, 4)), dma((table_n, 4)), dma((3,)), dma((3,)), dma((2 * table_n + 1,)),
        ],
        compiler_params=pltpu.CompilerParams(collective_id=1, has_side_effects=True, vmem_limit_bytes=VMEM_LIMIT),
        name="exchange",
    )(rows, x, dy, gt, ids)


def spread(row):
    n = row.shape[1]
    return jnp.concatenate([jnp.broadcast_to(row[:, c * 128:(c + 1) * 128], (128, 128)).T for c in range(n // 128)], axis=0)


def fill_kernel(pool, n_local, ids_ref, du_ref, dv_ref, dest_ref, list_ref, zero, zsem):
    tiles_n = du_ref.shape[0]
    fill = zero.shape[0]
    n = dest_ref.shape[1]
    zero[...] = jnp.zeros_like(zero)
    copies = []
    for ref in (du_ref, dv_ref):
        for i in range(tiles_n // fill):
            copies.append(pltpu.make_async_copy(zero, ref.at[pl.ds(i * fill, fill)], zsem.at[len(copies)]))
            copies[-1].start()

    per = LANES // pool
    first = lax.axis_index('table') * n_local
    lane = lax.broadcasted_iota(jnp.int32, (1, LANES), 1)
    table_n = ids_ref.shape[1]
    chunks = []
    for c in range(n // LANES):
        out = None
        for j in range(per):
            b = c * per + j
            piece = ids_ref[b // table_n, b % table_n]
            if j:
                piece = pltpu.roll(piece, j * pool, 1)
                out = jnp.where(lane >= j * pool, piece, out)
            else:
                out = piece
        chunks.append(out - first)
    ids_i = jnp.concatenate(chunks, axis=1)
    row = lax.shift_right_logical(ids_i, 3).astype(F32)
    line = jnp.bitwise_and(ids_i, 7).astype(F32)
    col = spread(row)
    k_row = lax.broadcasted_iota(jnp.int32, (1, n), 1).astype(F32)
    k_col = lax.broadcasted_iota(jnp.int32, (LANES, LANES), 0).astype(F32)

    def over(fn):
        outs = []
        for c in range(n // LANES):
            acc = jnp.zeros((8, LANES), F32)
            for b in range(n // LANES):
                acc = acc + fn(b, c).reshape(LANES // 8, 8, LANES).sum(0)
            outs.append(acc.sum(0, keepdims=True))
        return jnp.concatenate(outs, axis=1)

    def down(val, b):
        return val[b * LANES:(b + 1) * LANES, :]

    def side(val, c):
        return val[:, c * LANES:(c + 1) * LANES]

    leader = over(lambda b, c: jnp.where((down(col, b) == side(row, c)) & (k_col + float(b * LANES) < side(k_row, c)), 1.0, 0.0)) == 0.0
    lead_col = spread(jnp.where(leader, row, 1e9))
    rank = over(lambda b, c: jnp.where(down(lead_col, b) < side(row, c), 1.0, 0.0))
    dest_ref[...] = rank * 8.0 + line
    rank_col = spread(jnp.where(leader, rank, -1.0))
    tiles = over(lambda b, c: jnp.where(down(rank_col, b) == side(k_row, c), down(col, b), 0.0))
    count = jnp.sum(jnp.where(leader, 1.0, 0.0), axis=1, keepdims=True)
    for c in range(n // LANES):
        list_ref[c:c + 1, :] = side(tiles, c).astype(jnp.int32)
    list_ref[n // LANES:n // LANES + 8, :] = jnp.broadcast_to(count, (8, LANES)).astype(jnp.int32)
    for one in copies:
        one.wait()


def fill(ids, tiles_n, width, pool):
    n = ids.shape[0] * ids.shape[1] * pool
    vm = pl.BlockSpec(memory_space=pltpu.VMEM)
    hbm = pl.BlockSpec(memory_space=pl.ANY)
    step = 128
    return pl.pallas_call(
        functools.partial(fill_kernel, pool, tiles_n * 8),
        out_shape=(jax.ShapeDtypeStruct((tiles_n, 8, width), BF16),) * 2 + (jax.ShapeDtypeStruct((1, n), F32), jax.ShapeDtypeStruct((n // LANES + 8, LANES), jnp.int32)),
        in_specs=[vm],
        out_specs=(hbm, hbm, vm, vm),
        scratch_shapes=[pltpu.VMEM((step, 8, width), BF16), pltpu.SemaphoreType.DMA((2 * tiles_n // step,))],
        compiler_params=pltpu.CompilerParams(vmem_limit_bytes=VMEM_LIMIT),
        cost_estimate=pl.CostEstimate(flops=0, bytes_accessed=2 * tiles_n * 8 * width * 2, transcendentals=0),
        name="zero_tables",
    )(ids)


def tiles_kernel(list_ref, dest_ref, *refs):
    parts_u, parts_v = refs[0:4], refs[4:8]
    du_ref, dv_ref, stage, wsem = refs[10:14]
    n = dest_ref.shape[1]
    width = du_ref.shape[2]
    total = list_ref[n // LANES, 0]
    span = 256
    per = span // 8
    piece = n // 4
    target = lax.broadcasted_iota(jnp.int32, (span, n), 0).astype(F32)

    def build(c, carry):
        spot = target + (c * span).astype(F32)
        pick = jnp.where(spot == dest_ref[...], 1.0, 0.0).astype(BF16)
        for which, parts in enumerate((parts_u, parts_v)):
            acc = None
            for j in range(4):
                val = jnp.dot(pick[:, j * piece:(j + 1) * piece], parts[j][...].reshape(piece, width), preferred_element_type=F32)
                acc = val if acc is None else acc + val
            stage[which, pl.ds(c * per, per)] = acc.astype(BF16).reshape(per, 8, width)

        def put(q, inner):
            tile = list_ref[lax.div(q, LANES), lax.rem(q, LANES)]
            pltpu.make_async_copy(stage.at[0, q], du_ref.at[tile], wsem).start()
            pltpu.make_async_copy(stage.at[1, q], dv_ref.at[tile], wsem).start()
            return inner
        lax.fori_loop(c * per, jnp.minimum(total, (c + 1) * per), put, 0)
        return carry
    lax.fori_loop(0, lax.div(total + per - 1, per), build, 0)

    def put_wait(q, carry):
        pltpu.make_async_copy(stage.at[0, q], du_ref.at[0], wsem).wait()
        pltpu.make_async_copy(stage.at[1, q], dv_ref.at[0], wsem).wait()
        return carry
    lax.fori_loop(0, total, put_wait, 0)


def write_tiles(lst, dest, parts_u, parts_v, zero_u, zero_v):
    n = dest.shape[1]
    tiles_n, _, width = zero_u.shape
    vm = pl.BlockSpec(memory_space=pltpu.VMEM)
    hbm = pl.BlockSpec(memory_space=pl.ANY)
    return pl.pallas_call(
        tiles_kernel,
        out_shape=(jax.ShapeDtypeStruct((tiles_n, 8, width), BF16),) * 2,
        in_specs=[pl.BlockSpec(memory_space=pltpu.SMEM)] + [vm] * 9 + [hbm, hbm],
        out_specs=(hbm, hbm),
        scratch_shapes=[pltpu.VMEM((2, n, 8, width), BF16), pltpu.SemaphoreType.DMA],
        input_output_aliases={10: 0, 11: 1},
        compiler_params=pltpu.CompilerParams(vmem_limit_bytes=VMEM_LIMIT),
        name="write_tiles",
    )(lst, dest, *parts_u, *parts_v, zero_u, zero_v)


def solution(mesh):
    table_n = mesh.shape['table']
    data_n = mesh.shape['data']
    tok_spec = P(('replica', 'data', 'table'))
    row_spec = P(('replica', 'table'))
    up = [(i, (i + 1) % data_n) for i in range(data_n)]
    down = [(i, (i + data_n - 1) % data_n) for i in range(data_n)]

    def device_step(tok_loc, dy_loc, u_loc, v_loc, wanted_loc, pick_loc, gate_loc):
        n_local, width = u_loc.shape
        pool = wanted_loc.shape[1] // table_n
        tiles_n = n_local // 8
        ids, gt = share_ids(wanted_loc, pick_loc, gate_loc, table_n, pool)
        rows = fetch(ids, u_loc.reshape(tiles_n, 8, width), v_loc.reshape(tiles_n, 8, width), table_n, pool)
        y_loc, dx_loc, own_u, own_v, prev_u, prev_v, next_u, next_v, all_ids = exchange(rows, tok_loc, dy_loc, gt, ids, table_n, data_n, pool)
        far_u = lax.ppermute(prev_u, 'data', up)
        far_v = lax.ppermute(next_v, 'data', down)
        zero_u, zero_v, dest, lst = fill(all_ids, tiles_n, width, pool)
        grad_u, grad_v = write_tiles(lst, dest, (own_u, prev_u, next_u, far_u), (own_v, prev_v, next_v, far_v), zero_u, zero_v)
        return y_loc, dx_loc, grad_u.reshape(n_local, width), grad_v.reshape(n_local, width)

    return jax.shard_map(device_step, mesh=mesh, in_specs=(tok_spec, tok_spec, row_spec, row_spec, tok_spec, tok_spec, tok_spec), out_specs=(tok_spec, tok_spec, row_spec, row_spec), check_vma=False)
```

```python
import functools
import jax
import jax.numpy as jnp
from jax import lax
from jax.experimental import pallas as pl
from jax.experimental.pallas import tpu as pltpu
from jax.sharding import PartitionSpec as P

F32 = jnp.float32
BF16 = jnp.bfloat16
MIB = 1024 * 1024
MESH = pl.DeviceIdType.MESH
LANES = 128


def partner(index, k):
    out, bit = 0, 1
    while bit <= k or bit < 2:
        old = (index // bit) % 2
        out = out + ((1 - old) if k & bit else old) * bit
        bit *= 2
    return out + (index // bit) * bit


def visit_order(n):
    chips = max(1, n // 2)
    return sorted(range(n), key=lambda k: (max(min(abs(c - (c ^ (k // 2))), chips - abs(c - (c ^ (k // 2)))) for c in range(chips)), k))


def gelu_pair(pre_act):
    cdf_val = 0.5 * (1.0 + lax.erf(pre_act * 0.7071067811865476))
    pdf_val = jnp.exp(-0.5 * pre_act * pre_act) * 0.3989422804014327
    return pre_act * cdf_val, cdf_val + pre_act * pdf_val


def three_terms(val):
    hi = val.astype(BF16)
    rest = val - hi.astype(F32)
    mid = rest.astype(BF16)
    low = (rest - mid.astype(F32)).astype(BF16)
    return jnp.concatenate([hi, mid, low], axis=0)


def exact_dot(val, rhs):
    rows = val.shape[0]
    out = jnp.dot(three_terms(val), rhs, preferred_element_type=F32)
    return out[:rows] + out[rows:2 * rows] + out[2 * rows:]


def nt_dot(lhs, rhs):
    return lax.dot_general(lhs, rhs, (((1,), (1,)), ((), ())), preferred_element_type=F32)


def ids_kernel(table_n, pool, wanted_ref, ids_ref, out_buf, land, send_sem, recv_sem):
    me = lax.axis_index('table')
    others = range(1, table_n)
    barrier = pltpu.get_barrier_semaphore()
    for k in others:
        pl.semaphore_signal(barrier, inc=1, device_id={'table': partner(me, k)}, device_id_type=MESH)
    for e in range(table_n):
        out_buf[e, :, 0:pool] = wanted_ref[:, e * pool:(e + 1) * pool]
    land[0] = out_buf[me]
    pl.semaphore_wait(barrier, table_n - 1)
    copies = []
    for k in others:
        to = partner(me, k)
        copies.append(pltpu.make_async_remote_copy(src_ref=out_buf.at[to], dst_ref=land.at[k], send_sem=send_sem.at[k], recv_sem=recv_sem.at[k], device_id={'table': to}, device_id_type=MESH))
        copies[-1].start()
    for one in copies:
        one.wait()
    ids_ref[...] = land[...]


def share_ids(wanted, table_n, pool):
    vm = pl.BlockSpec(memory_space=pltpu.VMEM)
    return pl.pallas_call(
        functools.partial(ids_kernel, table_n, pool),
        out_shape=jax.ShapeDtypeStruct((table_n, 1, LANES), jnp.int32),
        in_specs=[vm],
        out_specs=vm,
        scratch_shapes=[
            pltpu.VMEM((table_n, 1, LANES), jnp.int32),
            pltpu.VMEM((table_n, 1, LANES), jnp.int32),
            pltpu.SemaphoreType.DMA((table_n,)),
            pltpu.SemaphoreType.DMA((table_n,)),
        ],
        compiler_params=pltpu.CompilerParams(collective_id=0, has_side_effects=True, vmem_limit_bytes=2 * MIB),
        name="share_ids",
    )(wanted)


def fetch_kernel(table_n, pool, n_local, ids_ref, u_ref, v_ref, rows_ref, tiles, sem):
    first = lax.axis_index('table') * n_local
    for k in range(table_n):
        for i in range(pool):
            tile = lax.shift_right_logical(ids_ref[k, 0, i] - first, 3)
            pltpu.make_async_copy(u_ref.at[tile], tiles.at[k, 0, i], sem.at[k]).start()
            pltpu.make_async_copy(v_ref.at[tile], tiles.at[k, 1, i], sem.at[k]).start()

    width = u_ref.shape[2]
    sub = lax.broadcasted_iota(jnp.int32, (8, width), 0)
    for k in range(table_n):
        pltpu.make_async_copy(tiles.at[k], tiles.at[k], sem.at[k]).wait()

        def pull(g, carry, k=k):
            for which in range(2):
                out = jnp.zeros((8, width), F32)
                for i in range(8):
                    s = g * 8 + i
                    line = jnp.bitwise_and(ids_ref[k, 0, s] - first, 7)
                    turned = pltpu.roll(tiles[k, which, s].astype(F32), jnp.bitwise_and(i - line + 8, 7), 0)
                    out = jnp.where(sub == i, turned, out)
                rows_ref[k, which, pl.ds(pl.multiple_of(g * 8, 8), 8), :] = out.astype(BF16)
            return carry
        lax.fori_loop(0, pool // 8, pull, 0)


def fetch(ids, u_tiles, v_tiles, table_n, pool):
    width = u_tiles.shape[2]
    hbm = pl.BlockSpec(memory_space=pl.ANY)
    return pl.pallas_call(
        functools.partial(fetch_kernel, table_n, pool, u_tiles.shape[0] * 8),
        out_shape=jax.ShapeDtypeStruct((table_n, 2, pool, width), BF16),
        in_specs=[pl.BlockSpec(memory_space=pltpu.SMEM), hbm, hbm],
        out_specs=pl.BlockSpec(memory_space=pltpu.VMEM),
        scratch_shapes=[pltpu.VMEM((table_n, 2, pool, 8, width), BF16), pltpu.SemaphoreType.DMA((table_n,))],
        compiler_params=pltpu.CompilerParams(vmem_limit_bytes=40 * MIB),
        name="fetch_rows",
    )(ids, u_tiles, v_tiles)


PLAN = "a1 a2 a6 a3 a7 s0 i0 w1 s1 w2 w6 a4 w3 w7 a5 s2 s6 s3 s7 w4 w5 x4 x5"


def plan_of(order, early):
    if order == [0, 1, 2, 3, 6, 7, 4, 5] and early == 6:
        return PLAN.split()
    others = order[1:]
    return [f"a{k}" for k in others] + ["s0", "i0"] + [f"w{k}" for k in others] + [("s" if k in order[:early] else "x") + str(k) for k in others]


def split_of(table_n):
    return table_n - table_n // 4


def exchange_kernel(table_n, data_n, pool, send_ref, x_ref, dy_ref, pick_ref, gate_ref, ids_ref,
                    w_all, c_all, rows_in, own_u, own_v, to_next, prev_v, next_u, to_prev, late, ids_out,
                    part,
                    a_send, a_recv, b_send, b_recv, c_send, c_recv, i_send, i_recv):
    me = lax.axis_index('table')
    row = lax.axis_index('data')
    after, before, across = (row + 1) % data_n, (row + data_n - 1) % data_n, (row + 2) % data_n
    order = visit_order(table_n)
    early = split_of(table_n)
    spot = {k: p for p, k in enumerate(order)}
    others = order[1:]
    along = (after, before, across)
    barrier = pltpu.get_barrier_semaphore()
    for k in others:
        pl.semaphore_signal(barrier, inc=1, device_id={'table': partner(me, k)}, device_id_type=MESH)
    for to in along:
        pl.semaphore_signal(barrier, inc=1, device_id={'data': to}, device_id_type=MESH)
    def remote(src, dst, sem_s, sem_r, **to):
        copy = pltpu.make_async_remote_copy(src_ref=src, dst_ref=dst, send_sem=sem_s, recv_sem=sem_r, device_id=to, device_id_type=MESH)
        copy.start()
        return copy

    copies_a, copies_b, copies_c = {}, {}, []
    x = x_ref[...]
    dy = dy_ref[...]

    def home(k, w):
        p = spot[k]
        return (own_u, own_v)[w].at[p] if p < early else late.at[w, p - early]

    def ask(k):
        copies_a[k] = remote(send_ref.at[k], rows_in.at[spot[k]], a_send.at[k], a_recv.at[k], table=partner(me, k))

    def share(k):
        for j, to in enumerate(along):
            copies_c.append(remote(ids_ref, ids_out.at[j + 1], i_send.at[j], i_recv.at[j], data=to))
        ids_out[0] = ids_ref[...]

    def gates_of(e):
        toks = x.shape[0]
        entry = (lax.broadcasted_iota(jnp.int32, (pool, toks), 0) + e * pool).astype(F32)
        accs = [jnp.zeros((pool, toks), F32) for _ in range(2)]

        def add_gate(i, accs):
            accs = list(accs)
            for j in range(16):
                s = i * 16 + j
                accs[j % 2] = accs[j % 2] + jnp.where(entry == pick_ref[pl.ds(s, 1), :].astype(F32), gate_ref[pl.ds(s, 1), :], 0.0)
            return tuple(accs)
        accs = lax.fori_loop(0, pick_ref.shape[0] // 16, add_gate, tuple(accs))
        return accs[0] + accs[1]

    def spread_on(k):
        p = spot[k]
        for w, (prev, nxt) in enumerate(((to_next, next_u), (prev_v, to_prev))):
            if k:
                copies_b[k, w].wait_recv()
            copies_c.append(remote(home(k, w), prev.at[p], c_send.at[k, w], c_recv.at[k, w], data=after))
            copies_c.append(remote(home(k, w), nxt.at[p], c_send.at[k, 2 + w], c_recv.at[k, 2 + w], data=before))

    def hold(k):
        p = spot[k] - early
        for w in range(2):
            copies_b[k, w].wait_recv()
            for out in (to_next, to_prev):
                out[early + w * (table_n - early) + p] = late[w, p]

    def work(k):
        e = partner(me, k)
        p = spot[k]
        gate = gates_of(e)
        if k:
            copies_a[k].wait_recv()
        else:
            rows_in[p] = send_ref[k]
        pre = nt_dot(rows_in[p, 0], x)
        v_dy = nt_dot(rows_in[p, 1], dy)
        act, slope = gelu_pair(pre)
        weight = gate * act
        coef = gate * slope * v_dy
        w_all[p * pool:(p + 1) * pool, :] = weight
        c_all[p * pool:(p + 1) * pool, :] = coef
        for w, val in enumerate((exact_dot(coef, x), exact_dot(weight, dy))):
            if k:
                part[k, w] = val.astype(BF16)
                copies_b[k, w] = remote(part.at[k, w], home(k, w), b_send.at[k, w], b_recv.at[k, w], table=e)
            else:
                home(k, w)[...] = val.astype(BF16)

    work(0)
    pl.semaphore_wait(barrier, len(others) + len(along))
    for step in plan_of(order, early):
        {'a': ask, 'w': work, 's': spread_on, 'x': hold, 'i': share}[step[0]](int(step[1:]))

    for k in others:
        copies_a[k].wait_send()
        copies_b[k, 0].wait_send()
        copies_b[k, 1].wait_send()
    for one in copies_c:
        one.wait()


def exchange(rows, x, dy, pick, gate, ids, table_n, data_n, pool):
    toks, width = x.shape
    entries = table_n * pool
    vm = pl.BlockSpec(memory_space=pltpu.VMEM)
    hbm = pl.BlockSpec(memory_space=pl.ANY)
    early = split_of(table_n)
    block = jax.ShapeDtypeStruct((early, pool, width), BF16)
    pack = jax.ShapeDtypeStruct((2 * table_n - early, pool, width), BF16)
    factor = jax.ShapeDtypeStruct((entries, toks), F32)
    both = (table_n, 2, pool, width)
    dma = pltpu.SemaphoreType.DMA
    return pl.pallas_call(
        functools.partial(exchange_kernel, table_n, data_n, pool),
        out_shape=(factor, factor, jax.ShapeDtypeStruct(both, BF16)) + (block, block, pack, block, block, pack) + (jax.ShapeDtypeStruct((2, table_n - early, pool, width), BF16), jax.ShapeDtypeStruct((4, table_n, 1, LANES), jnp.int32)),
        in_specs=[vm] * 6,
        out_specs=(vm,) * 11,
        scratch_shapes=[
            pltpu.VMEM(both, BF16),
            dma((table_n,)), dma((table_n,)), dma((table_n, 2)), dma((table_n, 2)),
            dma((table_n, 4)), dma((table_n, 4)), dma((3,)), dma((3,)),
        ],
        compiler_params=pltpu.CompilerParams(collective_id=1, has_side_effects=True, vmem_limit_bytes=16 * MIB),
        name="exchange",
    )(rows, x, dy, pick, gate, ids)


def blocks_of(table_n):
    order = visit_order(table_n)
    early, last = order[:split_of(table_n)], order[split_of(table_n):]
    near = [(0, k) for k in early + last] + [(s, k) for s in (1, 2) for k in early]
    return near + [(s, k) for s in (1, 2, 3) for k in last] + [(3, k) for k in early], len(near)


def stack(blocks):
    return jnp.concatenate([b.reshape(-1, b.shape[-1]) for b in blocks], axis=0)


def spread(row):
    n = row.shape[1]
    return jnp.concatenate([jnp.broadcast_to(row[:, c * 128:(c + 1) * 128], (128, 128)).T for c in range(n // 128)], axis=0)


def fill_kernel(pool, n_local, ids_ref, w_ref, c_ref, rows_ref, own_u, own_v, to_next, prev_v, next_u, to_prev, late,
                du_ref, dv_ref, y_ref, dx_ref, sum_u, sum_v, rank_ref, spot_ref, list_ref,
                zero, zsem):
    tiles_n = du_ref.shape[0]
    step = zero.shape[0]
    n = rank_ref.shape[1]
    width = du_ref.shape[2]
    zero[...] = jnp.zeros_like(zero)

    def start(i, carry):
        for w, ref in enumerate((du_ref, dv_ref)):
            pltpu.make_async_copy(zero, ref.at[pl.ds(i * step, step)], zsem.at[w]).start()
        return carry
    lax.fori_loop(0, tiles_n // step, start, 0)

    per = LANES // pool
    first = lax.axis_index('table') * n_local
    lane = lax.broadcasted_iota(jnp.int32, (1, LANES), 1)
    table_n = ids_ref.shape[1]
    blocks, n_near = blocks_of(table_n)
    near = n_near * pool
    chunks = []
    for c in range(n // LANES):
        out = None
        for j in range(per):
            piece = ids_ref[blocks[c * per + j]]
            if j:
                piece = pltpu.roll(piece, j * pool, 1)
                out = jnp.where(lane >= j * pool, piece, out)
            else:
                out = piece
        chunks.append(out - first)
    ids_i = jnp.concatenate(chunks, axis=1)
    row = ids_i.astype(F32)
    tile = lax.shift_right_logical(ids_i, 3).astype(F32)
    line = jnp.bitwise_and(ids_i, 7).astype(F32)
    row_col = spread(row)
    tile_col = spread(tile)
    k_row = lax.broadcasted_iota(jnp.int32, (1, n), 1).astype(F32)
    k_col = lax.broadcasted_iota(jnp.int32, (LANES, LANES), 0).astype(F32)

    def over(fn, wide=n):
        outs = []
        for c in range(wide // LANES):
            acc = jnp.zeros((8, LANES), F32)
            for b in range(n // LANES):
                acc = acc + fn(b, c).reshape(LANES // 8, 8, LANES).sum(0)
            outs.append(acc.sum(0, keepdims=True))
        return jnp.concatenate(outs, axis=1)

    def down(val, b):
        return val[b * LANES:(b + 1) * LANES, :]

    def side(val, c):
        return val[:, c * LANES:(c + 1) * LANES]

    def ranked(val, col):
        earlier = over(lambda b, c: jnp.where((down(col, b) == side(val, c)) & (k_col + float(b * LANES) < side(k_row, c)), 1.0, 0.0))
        leader = earlier == 0.0
        lead_col = spread(jnp.where(leader, val, 1e9))
        return leader, over(lambda b, c: jnp.where(down(lead_col, b) < side(val, c), 1.0, 0.0))

    row_leader, rank = ranked(row, row_col)
    tile_leader, tile_rank = ranked(tile, tile_col)
    rank_col = spread(jnp.where(row_leader, rank, -1.0))
    tile_rank_col = spread(jnp.where(tile_leader, tile_rank, -1.0))
    spot_col = spread(tile_rank * 8.0 + line)
    spots = over(lambda b, c: jnp.where(down(rank_col, b) == side(k_row, c), down(spot_col, b), 0.0))
    tiles = over(lambda b, c: jnp.where(down(tile_rank_col, b) == side(k_row, c), down(tile_col, b), 0.0))
    lead_spot_col = spread(jnp.where(row_leader, tile_rank * 8.0 + line, 1e9))
    before = over(lambda b, c: jnp.where(down(lead_spot_col, b) < side(k_row, c) * 256.0, 1.0, 0.0), LANES)
    n_rows = jnp.sum(jnp.where(row_leader, 1.0, 0.0))
    n_tiles = jnp.sum(jnp.where(tile_leader, 1.0, 0.0))
    rank_ref[...] = rank
    lines = n // LANES
    lane_f = lane.astype(F32)
    for c in range(lines):
        spot_ref[c:c + 1, :] = jnp.where(side(k_row, c) < n_rows, side(spots, c), -1.0)
        list_ref[c:c + 1, :] = side(tiles, c).astype(jnp.int32)
    list_ref[lines:lines + 1, :] = jnp.where(lane == 0, n_tiles, n_rows).astype(jnp.int32)
    list_ref[lines + 1:lines + 2, :] = before.astype(jnp.int32)
    list_ref[lines + 2:, :] = jnp.zeros((list_ref.shape[0] - lines - 2, LANES), jnp.int32)

    flat = (table_n * pool, width)
    y_ref[...] = exact_dot(w_ref[...].T, rows_ref[:, 1].reshape(flat)).astype(BF16)
    dx_ref[...] = exact_dot(c_ref[...].T, rows_ref[:, 0].reshape(flat)).astype(BF16)

    target = lax.broadcasted_iota(jnp.int32, (LANES, near), 0).astype(F32)
    n_chunks = lax.div(n_rows.astype(jnp.int32) + (LANES - 1), LANES)

    def add_up(c, carry):
        hot = jnp.where(target + (c * LANES).astype(F32) == rank_ref[:, 0:near], 1.0, 0.0).astype(BF16)
        span = pl.ds(pl.multiple_of(c * LANES, LANES), LANES)
        for w, (out, own, prev, nxt) in enumerate(((sum_u, own_u, to_next, next_u), (sum_v, own_v, prev_v, to_prev))):
            out[span, :] = jnp.dot(hot, stack([own[...], late[w], prev[0:own.shape[0]], nxt[0:own.shape[0]]]), preferred_element_type=F32)
        return carry
    lax.fori_loop(0, n_chunks, add_up, 0)
    for w, ref in enumerate((du_ref, dv_ref)):
        pltpu.make_async_copy(ref, ref, zsem.at[w]).wait()


def fill(ids, w_all, c_all, rows, near, tiles_n, pool):
    table_n = ids.shape[1]
    n = ids.shape[0] * table_n * pool
    entries, toks = w_all.shape
    width = rows.shape[3]
    vm = pl.BlockSpec(memory_space=pltpu.VMEM)
    hbm = pl.BlockSpec(memory_space=pl.ANY)
    step = 128
    tok_shape = jax.ShapeDtypeStruct((toks, width), BF16)
    return pl.pallas_call(
        functools.partial(fill_kernel, pool, tiles_n * 8),
        out_shape=(jax.ShapeDtypeStruct((tiles_n, 8, width), BF16),) * 2 + (tok_shape, tok_shape)
        + (jax.ShapeDtypeStruct((n, width), F32),) * 2
        + (jax.ShapeDtypeStruct((1, n), F32), jax.ShapeDtypeStruct((n // LANES, LANES), F32), jax.ShapeDtypeStruct((n // LANES + 8, LANES), jnp.int32)),
        in_specs=[vm] * 11,
        out_specs=(hbm, hbm) + (vm,) * 7,
        scratch_shapes=[
            pltpu.VMEM((step, 8, width), BF16),
            pltpu.SemaphoreType.DMA((2,)),
        ],
        compiler_params=pltpu.CompilerParams(vmem_limit_bytes=24 * MIB),
        cost_estimate=pl.CostEstimate(flops=0, bytes_accessed=2 * tiles_n * 8 * width * 2, transcendentals=0),
        name="zero_tables",
    )(ids, w_all, c_all, rows, *near)


def tiles_kernel(near, list_ref, rank_ref, spot_ref, from_prev, from_next, late_far, sum_u, sum_v, zero_u, zero_v, du_ref, dv_ref, done, stage, wsem):
    n = rank_ref.shape[1]
    width = du_ref.shape[2]
    lines = n // LANES
    n_tiles = list_ref[lines, 0]
    n_rows = list_ref[lines, 1]
    n_chunks = lax.div(n_rows + (LANES - 1), LANES)
    target = lax.broadcasted_iota(jnp.int32, (LANES, n - near), 0).astype(F32)

    def finish(c, carry):
        span = pl.ds(pl.multiple_of(c * LANES, LANES), LANES)
        hot = jnp.where(target + (c * LANES).astype(F32) == rank_ref[:, near:], 1.0, 0.0).astype(BF16)
        late_n = late_far.shape[1]
        early = from_prev.shape[0] - 2 * late_n
        for w, (far, sums) in enumerate(((from_prev, sum_u), (from_next, sum_v))):
            late = [ref[early + w * late_n:early + (w + 1) * late_n] for ref in (from_prev, from_next)]
            last = jnp.dot(hot, stack(late + [late_far[w], far[0:early]]), preferred_element_type=F32)
            done[w, span, :] = (sums[span, :] + last).astype(BF16)
        return carry
    lax.fori_loop(0, n_chunks, finish, 0)

    tall = 256
    per = tall // 8
    place = lax.broadcasted_iota(jnp.int32, (tall, LANES), 0).astype(F32)

    ring = stage.shape[0]
    n_builds = lax.div(n_tiles + per - 1, per)

    def drain(slot):
        pltpu.make_async_copy(stage.at[slot], stage.at[slot], wsem.at[slot]).wait()

    def build(c, carry):
        slot = lax.rem(c, ring)

        @pl.when(c >= ring)
        def _():
            drain(slot)
        start = lax.div(list_ref[lines + 1, c], LANES)
        end = lax.div(list_ref[lines + 1, c + 1] + (LANES - 1), LANES)

        def lay(kc):
            hot = jnp.where(place + (c * tall).astype(F32) == spot_ref[pl.ds(kc, 1), :], 1.0, 0.0).astype(BF16)
            span = pl.ds(pl.multiple_of(kc * LANES, LANES), LANES)
            return [jnp.dot(hot, done[w, span, :], preferred_element_type=F32).astype(BF16).reshape(per, 8, width) for w in range(2)]
        for w, val in enumerate(lay(start)):
            stage[slot, w] = val

        def more(kc, inner):
            for w, val in enumerate(lay(kc)):
                stage[slot, w] = stage[slot, w] + val
            return inner
        lax.fori_loop(start + 1, end, more, 0)

        def put(q, inner):
            tile = list_ref[lax.div(q, LANES), lax.rem(q, LANES)]
            pltpu.make_async_copy(stage.at[slot, 0, q - c * per], du_ref.at[tile], wsem.at[slot]).start()
            pltpu.make_async_copy(stage.at[slot, 1, q - c * per], dv_ref.at[tile], wsem.at[slot]).start()
            return inner
        lax.fori_loop(c * per, jnp.minimum(n_tiles, (c + 1) * per), put, 0)
        return carry
    lax.fori_loop(0, n_builds, build, 0)

    def full(c, carry):
        drain(lax.rem(c, ring))
        return carry
    lax.fori_loop(jnp.maximum(0, n_builds - ring), n_builds - 1, full, 0)
    slot = lax.rem(n_builds - 1, ring)

    def rest(q, carry):
        for w, ref in enumerate((du_ref, dv_ref)):
            pltpu.make_async_copy(stage.at[slot, w, 0], ref.at[0], wsem.at[slot]).wait()
        return carry
    lax.fori_loop((n_builds - 1) * per, n_tiles, rest, 0)


def write_tiles(lst, rank, spot, far, sum_u, sum_v, zero_u, zero_v, near):
    n = rank.shape[1]
    tiles_n, _, width = zero_u.shape
    vm = pl.BlockSpec(memory_space=pltpu.VMEM)
    hbm = pl.BlockSpec(memory_space=pl.ANY)
    return pl.pallas_call(
        functools.partial(tiles_kernel, near),
        out_shape=(jax.ShapeDtypeStruct((tiles_n, 8, width), BF16),) * 2,
        in_specs=[pl.BlockSpec(memory_space=pltpu.SMEM)] + [vm] * 7 + [hbm] * 2,
        out_specs=(hbm, hbm),
        scratch_shapes=[
            pltpu.VMEM((2, n, width), BF16),
            pltpu.VMEM((8, 2, 32, 8, width), BF16),
            pltpu.SemaphoreType.DMA((8,)),
        ],
        input_output_aliases={8: 0, 9: 1},
        compiler_params=pltpu.CompilerParams(vmem_limit_bytes=24 * MIB),
        name="write_tiles",
    )(lst, rank, spot, *far, sum_u, sum_v, zero_u, zero_v)


def solution(mesh):
    table_n = mesh.shape['table']
    data_n = mesh.shape['data']
    tok_spec = P(('replica', 'data', 'table'))
    row_spec = P(('replica', 'table'))
    up = [(i, (i + 1) % data_n) for i in range(data_n)]
    down = [(i, (i + data_n - 1) % data_n) for i in range(data_n)]
    over = [(i, (i + 2) % data_n) for i in range(data_n)]

    def device_step(tok_loc, dy_loc, u_loc, v_loc, wanted_loc, pick_loc, gate_loc):
        n_local, width = u_loc.shape
        toks = tok_loc.shape[0]
        pool = wanted_loc.shape[1] // table_n
        tiles_n = n_local // 8
        pick = pick_loc.transpose(1, 2, 0).reshape(-1, toks)
        gate = gate_loc.transpose(1, 2, 0).reshape(-1, toks)
        ids = share_ids(wanted_loc, table_n, pool)
        rows = fetch(ids, u_loc.reshape(tiles_n, 8, width), v_loc.reshape(tiles_n, 8, width), table_n, pool)
        w_all, c_all, rows_in, own_u, own_v, to_next, prev_v, next_u, to_prev, late, all_ids = exchange(rows, tok_loc, dy_loc, pick, gate, ids, table_n, data_n, pool)
        far = (lax.ppermute(to_next, 'data', up), lax.ppermute(to_prev, 'data', down), lax.ppermute(late, 'data', over))
        near = (own_u, own_v, to_next, prev_v, next_u, to_prev, late)
        zero_u, zero_v, y_loc, dx_loc, sum_u, sum_v, rank, spot, lst = fill(all_ids, w_all, c_all, rows_in, near, tiles_n, pool)
        grad_u, grad_v = write_tiles(lst, rank, spot, far, sum_u, sum_v, zero_u, zero_v, blocks_of(table_n)[1] * pool)
        return y_loc, dx_loc, grad_u.reshape(n_local, width), grad_v.reshape(n_local, width)

    return jax.shard_map(device_step, mesh=mesh, in_specs=(tok_spec, tok_spec, row_spec, row_spec, tok_spec, tok_spec, tok_spec), out_specs=(tok_spec, tok_spec, row_spec, row_spec), check_vma=False)
```

```python
import functools
import jax
import jax.numpy as jnp
from jax import lax
from jax.experimental import pallas as pl
from jax.experimental.pallas import tpu as pltpu
from jax.sharding import PartitionSpec as P

F32 = jnp.float32
BF16 = jnp.bfloat16
MIB = 1024 * 1024
MESH = pl.DeviceIdType.MESH
LANES = 128


def partner(index, k):
    out, bit = 0, 1
    while bit <= k or bit < 2:
        old = (index // bit) % 2
        out = out + ((1 - old) if k & bit else old) * bit
        bit *= 2
    return out + (index // bit) * bit


def visit_order(n):
    chips = max(1, n // 2)
    return sorted(range(n), key=lambda k: (max(min(abs(c - (c ^ (k // 2))), chips - abs(c - (c ^ (k // 2)))) for c in range(chips)), k))


def gelu_pair(pre_act):
    cdf_val = 0.5 * (1.0 + lax.erf(pre_act * 0.7071067811865476))
    pdf_val = jnp.exp(-0.5 * pre_act * pre_act) * 0.3989422804014327
    return pre_act * cdf_val, cdf_val + pre_act * pdf_val


def three_terms(val):
    hi = val.astype(BF16)
    rest = val - hi.astype(F32)
    mid = rest.astype(BF16)
    low = (rest - mid.astype(F32)).astype(BF16)
    return jnp.concatenate([hi, mid, low], axis=0)


def exact_dot(val, rhs):
    rows = val.shape[0]
    out = jnp.dot(three_terms(val), rhs, preferred_element_type=F32)
    return out[:rows] + out[rows:2 * rows] + out[2 * rows:]


def nt_dot(lhs, rhs):
    return lax.dot_general(lhs, rhs, (((1,), (1,)), ((), ())), preferred_element_type=F32)


def ids_kernel(table_n, pool, wanted_ref, ids_ref, out_buf, send_sem, recv_sem):
    me = lax.axis_index('table')
    others = range(1, table_n)
    barrier = pltpu.get_barrier_semaphore()
    for k in others:
        pl.semaphore_signal(barrier, inc=1, device_id={'table': partner(me, k)}, device_id_type=MESH)
    for e in range(table_n):
        out_buf[e, :, 0:pool] = wanted_ref[:, e * pool:(e + 1) * pool]
    ids_ref[0] = out_buf[me]
    pl.semaphore_wait(barrier, table_n - 1)
    copies = []
    for k in others:
        to = partner(me, k)
        copies.append(pltpu.make_async_remote_copy(src_ref=out_buf.at[to], dst_ref=ids_ref.at[k], send_sem=send_sem.at[k], recv_sem=recv_sem.at[k], device_id={'table': to}, device_id_type=MESH))
        copies[-1].start()
    for one in copies:
        one.wait()


def share_ids(wanted, table_n, pool):
    vm = pl.BlockSpec(memory_space=pltpu.VMEM)
    return pl.pallas_call(
        functools.partial(ids_kernel, table_n, pool),
        out_shape=jax.ShapeDtypeStruct((table_n, 1, LANES), jnp.int32),
        in_specs=[vm],
        out_specs=vm,
        scratch_shapes=[
            pltpu.VMEM((table_n, 1, LANES), jnp.int32),
            pltpu.SemaphoreType.DMA((table_n,)),
            pltpu.SemaphoreType.DMA((table_n,)),
        ],
        compiler_params=pltpu.CompilerParams(collective_id=0, has_side_effects=True, vmem_limit_bytes=2 * MIB),
        name="share_ids",
    )(wanted)


def fetch_kernel(table_n, pool, n_local, ids_ref, u_ref, v_ref, rows_ref, tiles, sem):
    first = lax.axis_index('table') * n_local
    for k in range(table_n):
        for i in range(pool):
            tile = lax.shift_right_logical(ids_ref[k, 0, i] - first, 3)
            pltpu.make_async_copy(u_ref.at[tile], tiles.at[k, 0, i], sem.at[k]).start()
            pltpu.make_async_copy(v_ref.at[tile], tiles.at[k, 1, i], sem.at[k]).start()

    width = u_ref.shape[2]
    sub = lax.broadcasted_iota(jnp.int32, (8, width), 0)
    for k in range(table_n):
        pltpu.make_async_copy(tiles.at[k], tiles.at[k], sem.at[k]).wait()

        def pull(g, carry, k=k):
            for which in range(2):
                out = jnp.zeros((8, width), F32)
                for i in range(8):
                    s = g * 8 + i
                    line = jnp.bitwise_and(ids_ref[k, 0, s] - first, 7)
                    turned = pltpu.roll(tiles[k, which, s].astype(F32), jnp.bitwise_and(i - line + 8, 7), 0)
                    out = jnp.where(sub == i, turned, out)
                rows_ref[k, which, pl.ds(pl.multiple_of(g * 8, 8), 8), :] = out.astype(BF16)
            return carry
        lax.fori_loop(0, pool // 8, pull, 0)


def fetch(ids, u_tiles, v_tiles, table_n, pool):
    width = u_tiles.shape[2]
    hbm = pl.BlockSpec(memory_space=pl.ANY)
    return pl.pallas_call(
        functools.partial(fetch_kernel, table_n, pool, u_tiles.shape[0] * 8),
        out_shape=jax.ShapeDtypeStruct((table_n, 2, pool, width), BF16),
        in_specs=[pl.BlockSpec(memory_space=pltpu.SMEM), hbm, hbm],
        out_specs=pl.BlockSpec(memory_space=pltpu.VMEM),
        scratch_shapes=[pltpu.VMEM((table_n, 2, pool, 8, width), BF16), pltpu.SemaphoreType.DMA((table_n,))],
        compiler_params=pltpu.CompilerParams(vmem_limit_bytes=40 * MIB),
        name="fetch_rows",
    )(ids, u_tiles, v_tiles)


PLAN = "a2 a6 a3 a1 a4 a7 w1 s0 i0 s1 w6 w3 w7 w2 s6 a5 s3 s7 s2 w4 w5 x4 x5"


def plan_of(order, early):
    if order == [0, 1, 2, 3, 6, 7, 4, 5] and early == 6:
        return PLAN.split()
    others = order[1:]
    return [f"a{k}" for k in others] + ["s0", "i0"] + [f"w{k}" for k in others] + [("s" if k in order[:early] else "x") + str(k) for k in others]


def split_of(table_n):
    return table_n - table_n // 4


def exchange_kernel(table_n, data_n, pool, send_ref, x_ref, dy_ref, pick_ref, gate_ref, ids_ref,
                    w_all, c_all, rows_in, own_u, own_v, to_next, prev_v, next_u, to_prev, late, ids_out,
                    part,
                    a_send, a_recv, b_send, b_recv, c_send, c_recv, i_send, i_recv):
    me = lax.axis_index('table')
    row = lax.axis_index('data')
    after, before, across = (row + 1) % data_n, (row + data_n - 1) % data_n, (row + 2) % data_n
    order = visit_order(table_n)
    early = split_of(table_n)
    spot = {k: p for p, k in enumerate(order)}
    others = order[1:]
    along = (after, before, across)
    barrier = pltpu.get_barrier_semaphore()
    for k in others:
        pl.semaphore_signal(barrier, inc=1, device_id={'table': partner(me, k)}, device_id_type=MESH)
    for to in along:
        pl.semaphore_signal(barrier, inc=1, device_id={'data': to}, device_id_type=MESH)
    def remote(src, dst, sem_s, sem_r, **to):
        copy = pltpu.make_async_remote_copy(src_ref=src, dst_ref=dst, send_sem=sem_s, recv_sem=sem_r, device_id=to, device_id_type=MESH)
        copy.start()
        return copy

    copies_a, copies_b, copies_c = {}, {}, []
    x = x_ref[...]
    dy = dy_ref[...]

    def home(k, w):
        p = spot[k]
        return (own_u, own_v)[w].at[p] if p < early else late.at[w, p - early]

    def ask(k):
        copies_a[k] = remote(send_ref.at[k], rows_in.at[spot[k]], a_send.at[k], a_recv.at[k], table=partner(me, k))

    def share(k):
        for j, to in enumerate(along):
            copies_c.append(remote(ids_ref, ids_out.at[j + 1], i_send.at[j], i_recv.at[j], data=to))
        ids_out[0] = ids_ref[...]

    def gates_of(e):
        toks = x.shape[0]
        entry = (lax.broadcasted_iota(jnp.int32, (pool, toks), 0) + e * pool).astype(F32)
        accs = [jnp.zeros((pool, toks), F32) for _ in range(2)]

        def add_gate(i, accs):
            accs = list(accs)
            for j in range(16):
                s = i * 16 + j
                accs[j % 2] = accs[j % 2] + jnp.where(entry == pick_ref[pl.ds(s, 1), :].astype(F32), gate_ref[pl.ds(s, 1), :], 0.0)
            return tuple(accs)
        accs = lax.fori_loop(0, pick_ref.shape[0] // 16, add_gate, tuple(accs))
        return accs[0] + accs[1]

    def spread_on(k):
        p = spot[k]
        for w, (prev, nxt) in enumerate(((to_next, next_u), (prev_v, to_prev))):
            if k:
                copies_b[k, w].wait_recv()
            copies_c.append(remote(home(k, w), prev.at[p], c_send.at[k, w], c_recv.at[k, w], data=after))
            copies_c.append(remote(home(k, w), nxt.at[p], c_send.at[k, 2 + w], c_recv.at[k, 2 + w], data=before))

    def hold(k):
        p = spot[k] - early
        for w in range(2):
            copies_b[k, w].wait_recv()
            for out in (to_next, to_prev):
                out[early + w * (table_n - early) + p] = late[w, p]

    def work(k):
        e = partner(me, k)
        p = spot[k]
        gate = gates_of(e)
        if k:
            copies_a[k].wait_recv()
        else:
            rows_in[p] = send_ref[k]
        pre = nt_dot(rows_in[p, 0], x)
        v_dy = nt_dot(rows_in[p, 1], dy)
        act, slope = gelu_pair(pre)
        weight = gate * act
        coef = gate * slope * v_dy
        w_all[p * pool:(p + 1) * pool, :] = weight
        c_all[p * pool:(p + 1) * pool, :] = coef
        for w, val in enumerate((exact_dot(coef, x), exact_dot(weight, dy))):
            if k:
                part[k, w] = val.astype(BF16)
                copies_b[k, w] = remote(part.at[k, w], home(k, w), b_send.at[k, w], b_recv.at[k, w], table=e)
            else:
                home(k, w)[...] = val.astype(BF16)

    work(0)
    pl.semaphore_wait(barrier, len(others) + len(along))
    for step in plan_of(order, early):
        {'a': ask, 'w': work, 's': spread_on, 'x': hold, 'i': share}[step[0]](int(step[1:]))

    for k in others:
        copies_a[k].wait_send()
        copies_b[k, 0].wait_send()
        copies_b[k, 1].wait_send()
    for one in copies_c:
        one.wait()


def exchange(rows, x, dy, pick, gate, ids, table_n, data_n, pool):
    toks, width = x.shape
    entries = table_n * pool
    vm = pl.BlockSpec(memory_space=pltpu.VMEM)
    hbm = pl.BlockSpec(memory_space=pl.ANY)
    early = split_of(table_n)
    block = jax.ShapeDtypeStruct((early, pool, width), BF16)
    pack = jax.ShapeDtypeStruct((2 * table_n - early, pool, width), BF16)
    factor = jax.ShapeDtypeStruct((entries, toks), F32)
    both = (table_n, 2, pool, width)
    dma = pltpu.SemaphoreType.DMA
    return pl.pallas_call(
        functools.partial(exchange_kernel, table_n, data_n, pool),
        out_shape=(factor, factor, jax.ShapeDtypeStruct(both, BF16)) + (block, block, pack, block, block, pack) + (jax.ShapeDtypeStruct((2, table_n - early, pool, width), BF16), jax.ShapeDtypeStruct((4, table_n, 1, LANES), jnp.int32)),
        in_specs=[vm] * 6,
        out_specs=(vm,) * 11,
        scratch_shapes=[
            pltpu.VMEM(both, BF16),
            dma((table_n,)), dma((table_n,)), dma((table_n, 2)), dma((table_n, 2)),
            dma((table_n, 4)), dma((table_n, 4)), dma((3,)), dma((3,)),
        ],
        compiler_params=pltpu.CompilerParams(collective_id=1, has_side_effects=True, vmem_limit_bytes=16 * MIB),
        name="exchange",
    )(rows, x, dy, pick, gate, ids)


def blocks_of(table_n):
    order = visit_order(table_n)
    early, last = order[:split_of(table_n)], order[split_of(table_n):]
    near = [(0, k) for k in early + last] + [(s, k) for s in (1, 2) for k in early]
    return near + [(s, k) for s in (1, 2, 3) for k in last] + [(3, k) for k in early], len(near)


def stack(blocks):
    return jnp.concatenate([b.reshape(-1, b.shape[-1]) for b in blocks], axis=0)


def spread(row):
    n = row.shape[1]
    return jnp.concatenate([jnp.broadcast_to(row[:, c * 128:(c + 1) * 128], (128, 128)).T for c in range(n // 128)], axis=0)


FILL = 128
REST = 3


def fill_kernel(pool, n_local, ids_ref, w_ref, c_ref, rows_ref, own_u, own_v, to_next, prev_v, next_u, to_prev, late,
                du_ref, dv_ref, y_ref, dx_ref, sum_u, sum_v, rank_ref, spot_ref, list_ref,
                zero, zsem):
    tiles_n = du_ref.shape[0]
    step = zero.shape[0]
    n = rank_ref.shape[1]
    width = du_ref.shape[2]
    zero[...] = jnp.zeros_like(zero)

    def start(i, carry):
        pltpu.make_async_copy(zero, du_ref.at[pl.ds(i * step, step)], zsem.at[0]).start()

        @pl.when(i < tiles_n // step - REST)
        def _():
            pltpu.make_async_copy(zero, dv_ref.at[pl.ds(i * step, step)], zsem.at[1]).start()
        return carry
    lax.fori_loop(0, tiles_n // step, start, 0)

    per = LANES // pool
    first = lax.axis_index('table') * n_local
    lane = lax.broadcasted_iota(jnp.int32, (1, LANES), 1)
    table_n = ids_ref.shape[1]
    blocks, n_near = blocks_of(table_n)
    near = n_near * pool
    chunks = []
    for c in range(n // LANES):
        out = None
        for j in range(per):
            piece = ids_ref[blocks[c * per + j]]
            if j:
                piece = pltpu.roll(piece, j * pool, 1)
                out = jnp.where(lane >= j * pool, piece, out)
            else:
                out = piece
        chunks.append(out - first)
    ids_i = jnp.concatenate(chunks, axis=1)
    row = ids_i.astype(F32)
    tile = lax.shift_right_logical(ids_i, 3).astype(F32)
    line = jnp.bitwise_and(ids_i, 7).astype(F32)
    row_col = spread(row)
    tile_col = spread(tile)
    k_row = lax.broadcasted_iota(jnp.int32, (1, n), 1).astype(F32)
    k_col = lax.broadcasted_iota(jnp.int32, (LANES, LANES), 0).astype(F32)

    def over(fn, wide=n):
        outs = []
        for c in range(wide // LANES):
            acc = jnp.zeros((8, LANES), F32)
            for b in range(n // LANES):
                acc = acc + fn(b, c).reshape(LANES // 8, 8, LANES).sum(0)
            outs.append(acc.sum(0, keepdims=True))
        return jnp.concatenate(outs, axis=1)

    def down(val, b):
        return val[b * LANES:(b + 1) * LANES, :]

    def side(val, c):
        return val[:, c * LANES:(c + 1) * LANES]

    def ranked(val, col):
        earlier = over(lambda b, c: jnp.where((down(col, b) == side(val, c)) & (k_col + float(b * LANES) < side(k_row, c)), 1.0, 0.0))
        leader = earlier == 0.0
        lead_col = spread(jnp.where(leader, val, 1e9))
        return leader, over(lambda b, c: jnp.where(down(lead_col, b) < side(val, c), 1.0, 0.0))

    row_leader, rank = ranked(row, row_col)
    tile_leader, tile_rank = ranked(tile, tile_col)
    rank_col = spread(jnp.where(row_leader, rank, -1.0))
    tile_rank_col = spread(jnp.where(tile_leader, tile_rank, -1.0))
    spot_col = spread(tile_rank * 8.0 + line)
    spots = over(lambda b, c: jnp.where(down(rank_col, b) == side(k_row, c), down(spot_col, b), 0.0))
    tiles = over(lambda b, c: jnp.where(down(tile_rank_col, b) == side(k_row, c), down(tile_col, b), 0.0))
    lead_spot_col = spread(jnp.where(row_leader, tile_rank * 8.0 + line, 1e9))
    before = over(lambda b, c: jnp.where(down(lead_spot_col, b) < side(k_row, c) * 256.0, 1.0, 0.0), LANES)
    n_rows = jnp.sum(jnp.where(row_leader, 1.0, 0.0))
    n_tiles = jnp.sum(jnp.where(tile_leader, 1.0, 0.0))
    rank_ref[...] = rank
    lines = n // LANES
    lane_f = lane.astype(F32)
    for c in range(lines):
        spot_ref[c:c + 1, :] = jnp.where(side(k_row, c) < n_rows, side(spots, c), -1.0)
        list_ref[c:c + 1, :] = side(tiles, c).astype(jnp.int32)
    list_ref[lines:lines + 1, :] = jnp.where(lane == 0, n_tiles, n_rows).astype(jnp.int32)
    list_ref[lines + 1:lines + 2, :] = before.astype(jnp.int32)
    list_ref[lines + 2:, :] = jnp.zeros((list_ref.shape[0] - lines - 2, LANES), jnp.int32)

    flat = (table_n * pool, width)
    y_ref[...] = exact_dot(w_ref[...].T, rows_ref[:, 1].reshape(flat)).astype(BF16)
    dx_ref[...] = exact_dot(c_ref[...].T, rows_ref[:, 0].reshape(flat)).astype(BF16)

    target = lax.broadcasted_iota(jnp.int32, (LANES, near), 0).astype(F32)
    n_chunks = lax.div(n_rows.astype(jnp.int32) + (LANES - 1), LANES)

    def add_up(c, carry):
        hot = jnp.where(target + (c * LANES).astype(F32) == rank_ref[:, 0:near], 1.0, 0.0).astype(BF16)
        span = pl.ds(pl.multiple_of(c * LANES, LANES), LANES)
        for w, (out, own, prev, nxt) in enumerate(((sum_u, own_u, to_next, next_u), (sum_v, own_v, prev_v, to_prev))):
            out[span, :] = jnp.dot(hot, stack([own[...], late[w], prev[0:own.shape[0]], nxt[0:own.shape[0]]]), preferred_element_type=F32)
        return carry
    lax.fori_loop(0, n_chunks, add_up, 0)
    filled = dv_ref.at[pl.ds(0, tiles_n - REST * step)]
    pltpu.make_async_copy(du_ref, du_ref, zsem.at[0]).wait()
    pltpu.make_async_copy(filled, filled, zsem.at[1]).wait()


def fill(ids, w_all, c_all, rows, near, tiles_n, pool):
    table_n = ids.shape[1]
    n = ids.shape[0] * table_n * pool
    entries, toks = w_all.shape
    width = rows.shape[3]
    vm = pl.BlockSpec(memory_space=pltpu.VMEM)
    hbm = pl.BlockSpec(memory_space=pl.ANY)
    step = FILL
    tok_shape = jax.ShapeDtypeStruct((toks, width), BF16)
    return pl.pallas_call(
        functools.partial(fill_kernel, pool, tiles_n * 8),
        out_shape=(jax.ShapeDtypeStruct((tiles_n, 8, width), BF16),) * 2 + (tok_shape, tok_shape)
        + (jax.ShapeDtypeStruct((n, width), F32),) * 2
        + (jax.ShapeDtypeStruct((1, n), F32), jax.ShapeDtypeStruct((n // LANES, LANES), F32), jax.ShapeDtypeStruct((n // LANES + 8, LANES), jnp.int32)),
        in_specs=[vm] * 11,
        out_specs=(hbm, hbm) + (vm,) * 7,
        scratch_shapes=[
            pltpu.VMEM((step, 8, width), BF16),
            pltpu.SemaphoreType.DMA((2,)),
        ],
        compiler_params=pltpu.CompilerParams(vmem_limit_bytes=24 * MIB),
        cost_estimate=pl.CostEstimate(flops=0, bytes_accessed=2 * tiles_n * 8 * width * 2, transcendentals=0),
        name="zero_tables",
    )(ids, w_all, c_all, rows, *near)


def tiles_kernel(near, list_ref, rank_ref, spot_ref, from_prev, from_next, late_far, sum_u, sum_v, zero_u, zero_v, du_ref, dv_ref, done, stage, zero, wsem, zsem):
    n = rank_ref.shape[1]
    width = du_ref.shape[2]
    lines = n // LANES
    n_tiles = list_ref[lines, 0]
    n_rows = list_ref[lines, 1]
    n_chunks = lax.div(n_rows + (LANES - 1), LANES)
    step = zero.shape[0]
    left = FILL * REST
    kept = du_ref.shape[0] - left
    zero[...] = jnp.zeros_like(zero)

    def start(i, carry):
        pltpu.make_async_copy(zero, dv_ref.at[pl.ds(kept + i * step, step)], zsem).start()
        return carry
    lax.fori_loop(0, left // step, start, 0)

    target = lax.broadcasted_iota(jnp.int32, (LANES, n - near), 0).astype(F32)

    def finish(c, carry):
        span = pl.ds(pl.multiple_of(c * LANES, LANES), LANES)
        hot = jnp.where(target + (c * LANES).astype(F32) == rank_ref[:, near:], 1.0, 0.0).astype(BF16)
        late_n = late_far.shape[1]
        early = from_prev.shape[0] - 2 * late_n
        for w, (far, sums) in enumerate(((from_prev, sum_u), (from_next, sum_v))):
            late = [ref[early + w * late_n:early + (w + 1) * late_n] for ref in (from_prev, from_next)]
            last = jnp.dot(hot, stack(late + [late_far[w], far[0:early]]), preferred_element_type=F32)
            done[w, span, :] = (sums[span, :] + last).astype(BF16)
        return carry
    lax.fori_loop(0, n_chunks, finish, 0)

    tall = 256
    per = tall // 8
    place = lax.broadcasted_iota(jnp.int32, (tall, LANES), 0).astype(F32)

    ring = stage.shape[0]
    n_builds = lax.div(n_tiles + per - 1, per)

    def drain(slot):
        pltpu.make_async_copy(stage.at[slot], stage.at[slot], wsem.at[slot]).wait()

    def build(c, carry):
        slot = lax.rem(c, ring)
        start = lax.div(list_ref[lines + 1, c], LANES)
        end = lax.div(list_ref[lines + 1, c + 1] + (LANES - 1), LANES)

        def lay(kc):
            hot = jnp.where(place + (c * tall).astype(F32) == spot_ref[pl.ds(kc, 1), :], 1.0, 0.0).astype(BF16)
            span = pl.ds(pl.multiple_of(kc * LANES, LANES), LANES)
            return [jnp.dot(hot, done[w, span, :], preferred_element_type=F32).astype(BF16).reshape(per, 8, width) for w in range(2)]
        for w, val in enumerate(lay(start)):
            stage[slot, w] = val

        def more(kc, inner):
            for w, val in enumerate(lay(kc)):
                stage[slot, w] = stage[slot, w] + val
            return inner
        lax.fori_loop(start + 1, end, more, 0)
        return carry

    def put(c, w, ref):
        slot = lax.rem(c, ring)
        line = lax.div(c * per, LANES)
        base = lax.rem(c * per, LANES)
        count = n_tiles - c * per

        def one(i, carry):
            pltpu.make_async_copy(stage.at[slot, w, i], ref.at[list_ref[line, base + i]], wsem.at[slot]).start()
            return carry

        @pl.when(count >= per)
        def _():
            for i in range(per):
                one(i, 0)

        @pl.when(count < per)
        def _():
            lax.fori_loop(0, count, one, 0)

    def first(c, carry):
        build(c, 0)
        put(c, 0, du_ref)
        return carry
    lax.fori_loop(0, jnp.minimum(n_builds, ring), first, 0)
    tail = dv_ref.at[pl.ds(kept, left)]
    pltpu.make_async_copy(tail, tail, zsem).wait()

    def second(c, carry):
        put(c, 1, dv_ref)
        return carry
    lax.fori_loop(0, jnp.minimum(n_builds, ring), second, 0)

    def later(c, carry):
        drain(lax.rem(c, ring))
        build(c, 0)
        put(c, 0, du_ref)
        put(c, 1, dv_ref)
        return carry
    lax.fori_loop(ring, n_builds, later, 0)

    def full(c, carry):
        drain(lax.rem(c, ring))
        return carry
    lax.fori_loop(jnp.maximum(0, n_builds - ring), n_builds - 1, full, 0)
    slot = lax.rem(n_builds - 1, ring)

    def rest(q, carry):
        for w, ref in enumerate((du_ref, dv_ref)):
            pltpu.make_async_copy(stage.at[slot, w, 0], ref.at[0], wsem.at[slot]).wait()
        return carry
    lax.fori_loop((n_builds - 1) * per, n_tiles, rest, 0)


def write_tiles(lst, rank, spot, far, sum_u, sum_v, zero_u, zero_v, near):
    n = rank.shape[1]
    tiles_n, _, width = zero_u.shape
    vm = pl.BlockSpec(memory_space=pltpu.VMEM)
    hbm = pl.BlockSpec(memory_space=pl.ANY)
    return pl.pallas_call(
        functools.partial(tiles_kernel, near),
        out_shape=(jax.ShapeDtypeStruct((tiles_n, 8, width), BF16),) * 2,
        in_specs=[pl.BlockSpec(memory_space=pltpu.SMEM)] + [vm] * 7 + [hbm] * 2,
        out_specs=(hbm, hbm),
        scratch_shapes=[
            pltpu.VMEM((2, n, width), BF16),
            pltpu.VMEM((8, 2, 32, 8, width), BF16),
            pltpu.VMEM((FILL // 2, 8, width), BF16),
            pltpu.SemaphoreType.DMA((8,)),
            pltpu.SemaphoreType.DMA,
        ],
        input_output_aliases={8: 0, 9: 1},
        compiler_params=pltpu.CompilerParams(vmem_limit_bytes=24 * MIB),
        name="write_tiles",
    )(lst, rank, spot, *far, sum_u, sum_v, zero_u, zero_v)


def solution(mesh):
    table_n = mesh.shape['table']
    data_n = mesh.shape['data']
    tok_spec = P(('replica', 'data', 'table'))
    row_spec = P(('replica', 'table'))
    up = [(i, (i + 1) % data_n) for i in range(data_n)]
    down = [(i, (i + data_n - 1) % data_n) for i in range(data_n)]
    over = [(i, (i + 2) % data_n) for i in range(data_n)]

    def device_step(tok_loc, dy_loc, u_loc, v_loc, wanted_loc, pick_loc, gate_loc):
        n_local, width = u_loc.shape
        toks = tok_loc.shape[0]
        pool = wanted_loc.shape[1] // table_n
        tiles_n = n_local // 8
        pick = pick_loc.transpose(1, 2, 0).reshape(-1, toks)
        gate = gate_loc.transpose(1, 2, 0).reshape(-1, toks)
        ids = share_ids(wanted_loc, table_n, pool)
        rows = fetch(ids, u_loc.reshape(tiles_n, 8, width), v_loc.reshape(tiles_n, 8, width), table_n, pool)
        w_all, c_all, rows_in, own_u, own_v, to_next, prev_v, next_u, to_prev, late, all_ids = exchange(rows, tok_loc, dy_loc, pick, gate, ids, table_n, data_n, pool)
        far = (lax.ppermute(to_next, 'data', up), lax.ppermute(to_prev, 'data', down), lax.ppermute(late, 'data', over))
        near = (own_u, own_v, to_next, prev_v, next_u, to_prev, late)
        zero_u, zero_v, y_loc, dx_loc, sum_u, sum_v, rank, spot, lst = fill(all_ids, w_all, c_all, rows_in, near, tiles_n, pool)
        grad_u, grad_v = write_tiles(lst, rank, spot, far, sum_u, sum_v, zero_u, zero_v, blocks_of(table_n)[1] * pool)
        return y_loc, dx_loc, grad_u.reshape(n_local, width), grad_v.reshape(n_local, width)

    return jax.shard_map(device_step, mesh=mesh, in_specs=(tok_spec, tok_spec, row_spec, row_spec, tok_spec, tok_spec, tok_spec), out_specs=(tok_spec, tok_spec, row_spec, row_spec), check_vma=False)
```

```python
import functools
import jax
import jax.numpy as jnp
from jax import lax
from jax.experimental import pallas as pl
from jax.experimental.pallas import tpu as pltpu
from jax.sharding import PartitionSpec as P

F32 = jnp.float32
BF16 = jnp.bfloat16
MIB = 1024 * 1024
MESH = pl.DeviceIdType.MESH
LANES = 128


def partner(index, k):
    out, bit = 0, 1
    while bit <= k or bit < 2:
        old = (index // bit) % 2
        out = out + ((1 - old) if k & bit else old) * bit
        bit *= 2
    return out + (index // bit) * bit


def visit_order(n):
    chips = max(1, n // 2)
    return sorted(range(n), key=lambda k: (max(min(abs(c - (c ^ (k // 2))), chips - abs(c - (c ^ (k // 2)))) for c in range(chips)), k))


def gelu_pair(pre_act):
    cdf_val = 0.5 * (1.0 + lax.erf(pre_act * 0.7071067811865476))
    pdf_val = jnp.exp(-0.5 * pre_act * pre_act) * 0.3989422804014327
    return pre_act * cdf_val, cdf_val + pre_act * pdf_val


def three_terms(val):
    hi = val.astype(BF16)
    rest = val - hi.astype(F32)
    mid = rest.astype(BF16)
    low = (rest - mid.astype(F32)).astype(BF16)
    return jnp.concatenate([hi, mid, low], axis=0)


def exact_dot(val, rhs):
    rows = val.shape[0]
    out = jnp.dot(three_terms(val), rhs, preferred_element_type=F32)
    return out[:rows] + out[rows:2 * rows] + out[2 * rows:]


def nt_dot(lhs, rhs):
    return lax.dot_general(lhs, rhs, (((1,), (1,)), ((), ())), preferred_element_type=F32)


def ids_kernel(table_n, pool, wanted_ref, ids_ref, out_buf, send_sem, recv_sem):
    me = lax.axis_index('table')
    others = range(1, table_n)
    barrier = pltpu.get_barrier_semaphore()
    for k in others:
        pl.semaphore_signal(barrier, inc=1, device_id={'table': partner(me, k)}, device_id_type=MESH)
    for e in range(table_n):
        out_buf[e, :, 0:pool] = wanted_ref[:, e * pool:(e + 1) * pool]
    ids_ref[0] = out_buf[me]
    pl.semaphore_wait(barrier, table_n - 1)
    copies = []
    for k in others:
        to = partner(me, k)
        copies.append(pltpu.make_async_remote_copy(src_ref=out_buf.at[to], dst_ref=ids_ref.at[k], send_sem=send_sem.at[k], recv_sem=recv_sem.at[k], device_id={'table': to}, device_id_type=MESH))
        copies[-1].start()
    for one in copies:
        one.wait()


def share_ids(wanted, table_n, pool):
    vm = pl.BlockSpec(memory_space=pltpu.VMEM)
    return pl.pallas_call(
        functools.partial(ids_kernel, table_n, pool),
        out_shape=jax.ShapeDtypeStruct((table_n, 1, LANES), jnp.int32),
        in_specs=[vm],
        out_specs=vm,
        scratch_shapes=[
            pltpu.VMEM((table_n, 1, LANES), jnp.int32),
            pltpu.SemaphoreType.DMA((table_n,)),
            pltpu.SemaphoreType.DMA((table_n,)),
        ],
        compiler_params=pltpu.CompilerParams(collective_id=0, has_side_effects=True, vmem_limit_bytes=2 * MIB),
        name="share_ids",
    )(wanted)


def fetch_kernel(table_n, pool, n_local, ids_ref, u_ref, v_ref, rows_ref, tiles, sem):
    first = lax.axis_index('table') * n_local
    for k in range(table_n):
        for i in range(pool):
            tile = lax.shift_right_logical(ids_ref[k, 0, i] - first, 3)
            pltpu.make_async_copy(u_ref.at[tile], tiles.at[k, 0, i], sem.at[k]).start()
            pltpu.make_async_copy(v_ref.at[tile], tiles.at[k, 1, i], sem.at[k]).start()

    width = u_ref.shape[2]
    sub = lax.broadcasted_iota(jnp.int32, (8, width), 0)
    for k in range(table_n):
        pltpu.make_async_copy(tiles.at[k], tiles.at[k], sem.at[k]).wait()

        def pull(g, carry, k=k):
            for which in range(2):
                out = jnp.zeros((8, width), F32)
                for i in range(8):
                    s = g * 8 + i
                    line = jnp.bitwise_and(ids_ref[k, 0, s] - first, 7)
                    turned = pltpu.roll(tiles[k, which, s].astype(F32), jnp.bitwise_and(i - line + 8, 7), 0)
                    out = jnp.where(sub == i, turned, out)
                rows_ref[k, which, g * 8:(g + 1) * 8, :] = out.astype(BF16)
            return carry
        for g in range(pool // 8):
            pull(g, 0)


def fetch(ids, u_tiles, v_tiles, table_n, pool):
    width = u_tiles.shape[2]
    hbm = pl.BlockSpec(memory_space=pl.ANY)
    return pl.pallas_call(
        functools.partial(fetch_kernel, table_n, pool, u_tiles.shape[0] * 8),
        out_shape=jax.ShapeDtypeStruct((table_n, 2, pool, width), BF16),
        in_specs=[pl.BlockSpec(memory_space=pltpu.SMEM), hbm, hbm],
        out_specs=pl.BlockSpec(memory_space=pltpu.VMEM),
        scratch_shapes=[pltpu.VMEM((table_n, 2, pool, 8, width), BF16), pltpu.SemaphoreType.DMA((table_n,))],
        compiler_params=pltpu.CompilerParams(vmem_limit_bytes=40 * MIB),
        name="fetch_rows",
    )(ids, u_tiles, v_tiles)


PLAN = "a2 a6 a3 a7 a1 a4 s0 w1 s1 w6 w2 i0 w3 w7 s6 s2 a5 s3 s7 w4 w5 x4 x5"


def plan_of(order, early):
    if order == [0, 1, 2, 3, 6, 7, 4, 5] and early == 6:
        return PLAN.split()
    others = order[1:]
    return [f"a{k}" for k in others] + ["s0", "i0"] + [f"w{k}" for k in others] + [("s" if k in order[:early] else "x") + str(k) for k in others]


def split_of(table_n):
    return table_n - table_n // 4


def exchange_kernel(table_n, data_n, pool, send_ref, x_ref, dy_ref, pick_ref, gate_ref, ids_ref,
                    w_all, c_all, rows_in, own_u, own_v, to_next, prev_v, next_u, to_prev, late, ids_out,
                    part,
                    a_send, a_recv, b_send, b_recv, c_send, c_recv, i_send, i_recv):
    me = lax.axis_index('table')
    row = lax.axis_index('data')
    after, before, across = (row + 1) % data_n, (row + data_n - 1) % data_n, (row + 2) % data_n
    order = visit_order(table_n)
    early = split_of(table_n)
    spot = {k: p for p, k in enumerate(order)}
    others = order[1:]
    along = (after, before, across)
    barrier = pltpu.get_barrier_semaphore()
    for k in others:
        pl.semaphore_signal(barrier, inc=1, device_id={'table': partner(me, k)}, device_id_type=MESH)
    for to in along:
        pl.semaphore_signal(barrier, inc=1, device_id={'data': to}, device_id_type=MESH)
    def remote(src, dst, sem_s, sem_r, **to):
        copy = pltpu.make_async_remote_copy(src_ref=src, dst_ref=dst, send_sem=sem_s, recv_sem=sem_r, device_id=to, device_id_type=MESH)
        copy.start()
        return copy

    copies_a, copies_b, copies_c = {}, {}, []
    x = x_ref[...]
    dy = dy_ref[...]

    def home(k, w):
        p = spot[k]
        return (own_u, own_v)[w].at[p] if p < early else late.at[w, p - early]

    def ask(k):
        copies_a[k] = remote(send_ref.at[k], rows_in.at[spot[k]], a_send.at[k], a_recv.at[k], table=partner(me, k))

    def share(k):
        for j, to in enumerate(along):
            copies_c.append(remote(ids_ref, ids_out.at[j + 1], i_send.at[j], i_recv.at[j], data=to))
        ids_out[0] = ids_ref[...]

    def gates_of(e):
        toks = x.shape[0]
        entry = (lax.broadcasted_iota(jnp.int32, (pool, toks), 0) + e * pool).astype(F32)
        accs = [jnp.zeros((pool, toks), F32) for _ in range(2)]

        def add_gate(i, accs):
            accs = list(accs)
            for j in range(16):
                s = i * 16 + j
                accs[j % 2] = accs[j % 2] + jnp.where(entry == pick_ref[pl.ds(s, 1), :].astype(F32), gate_ref[pl.ds(s, 1), :], 0.0)
            return tuple(accs)
        accs = lax.fori_loop(0, pick_ref.shape[0] // 16, add_gate, tuple(accs))
        return accs[0] + accs[1]

    def spread_on(k):
        p = spot[k]
        for w, (prev, nxt) in enumerate(((to_next, next_u), (prev_v, to_prev))):
            if k:
                copies_b[k, w].wait_recv()
            copies_c.append(remote(home(k, w), prev.at[p], c_send.at[k, w], c_recv.at[k, w], data=after))
            copies_c.append(remote(home(k, w), nxt.at[p], c_send.at[k, 2 + w], c_recv.at[k, 2 + w], data=before))

    def hold(k):
        p = spot[k] - early
        for w in range(2):
            copies_b[k, w].wait_recv()
            for out in (to_next, to_prev):
                out[early + w * (table_n - early) + p] = late[w, p]

    def work(k):
        e = partner(me, k)
        p = spot[k]
        gate = gates_of(e)
        if k:
            copies_a[k].wait_recv()
        else:
            rows_in[p] = send_ref[k]
        pre = nt_dot(rows_in[p, 0], x)
        v_dy = nt_dot(rows_in[p, 1], dy)
        act, slope = gelu_pair(pre)
        weight = gate * act
        coef = gate * slope * v_dy
        w_all[p * pool:(p + 1) * pool, :] = weight
        c_all[p * pool:(p + 1) * pool, :] = coef
        for w, val in enumerate((exact_dot(coef, x), exact_dot(weight, dy))):
            if k:
                part[k, w] = val.astype(BF16)
                copies_b[k, w] = remote(part.at[k, w], home(k, w), b_send.at[k, w], b_recv.at[k, w], table=e)
            else:
                home(k, w)[...] = val.astype(BF16)

    work(0)
    pl.semaphore_wait(barrier, len(others) + len(along))
    for step in plan_of(order, early):
        {'a': ask, 'w': work, 's': spread_on, 'x': hold, 'i': share}[step[0]](int(step[1:]))

    for k in others:
        copies_a[k].wait_send()
        copies_b[k, 0].wait_send()
        copies_b[k, 1].wait_send()
    for one in copies_c:
        one.wait()


def exchange(rows, x, dy, pick, gate, ids, table_n, data_n, pool):
    toks, width = x.shape
    entries = table_n * pool
    vm = pl.BlockSpec(memory_space=pltpu.VMEM)
    hbm = pl.BlockSpec(memory_space=pl.ANY)
    early = split_of(table_n)
    block = jax.ShapeDtypeStruct((early, pool, width), BF16)
    pack = jax.ShapeDtypeStruct((2 * table_n - early, pool, width), BF16)
    factor = jax.ShapeDtypeStruct((entries, toks), F32)
    both = (table_n, 2, pool, width)
    dma = pltpu.SemaphoreType.DMA
    return pl.pallas_call(
        functools.partial(exchange_kernel, table_n, data_n, pool),
        out_shape=(factor, factor, jax.ShapeDtypeStruct(both, BF16)) + (block, block, pack, block, block, pack) + (jax.ShapeDtypeStruct((2, table_n - early, pool, width), BF16), jax.ShapeDtypeStruct((4, table_n, 1, LANES), jnp.int32)),
        in_specs=[vm] * 6,
        out_specs=(vm,) * 11,
        scratch_shapes=[
            pltpu.VMEM(both, BF16),
            dma((table_n,)), dma((table_n,)), dma((table_n, 2)), dma((table_n, 2)),
            dma((table_n, 4)), dma((table_n, 4)), dma((3,)), dma((3,)),
        ],
        compiler_params=pltpu.CompilerParams(collective_id=1, has_side_effects=True, vmem_limit_bytes=16 * MIB),
        name="exchange",
    )(rows, x, dy, pick, gate, ids)


def blocks_of(table_n):
    order = visit_order(table_n)
    early, last = order[:split_of(table_n)], order[split_of(table_n):]
    near = [(0, k) for k in early + last] + [(s, k) for s in (1, 2) for k in early]
    return near + [(s, k) for s in (1, 2, 3) for k in last] + [(3, k) for k in early], len(near)


def stack(blocks):
    return jnp.concatenate([b.reshape(-1, b.shape[-1]) for b in blocks], axis=0)


def spread(row):
    n = row.shape[1]
    return jnp.concatenate([jnp.broadcast_to(row[:, c * 128:(c + 1) * 128], (128, 128)).T for c in range(n // 128)], axis=0)


FILL = 128
REST = 3


def fill_kernel(pool, n_local, ids_ref, w_ref, c_ref, rows_ref, own_u, own_v, to_next, prev_v, next_u, to_prev, late,
                du_ref, dv_ref, y_ref, dx_ref, sum_u, sum_v, rank_ref, spot_ref, list_ref,
                zero, zsem):
    tiles_n = du_ref.shape[0]
    step = zero.shape[0]
    n = rank_ref.shape[1]
    width = du_ref.shape[2]
    zero[...] = jnp.zeros_like(zero)

    def start(i, carry):
        pltpu.make_async_copy(zero, du_ref.at[pl.ds(i * step, step)], zsem.at[0]).start()

        @pl.when(i < tiles_n // step - REST)
        def _():
            pltpu.make_async_copy(zero, dv_ref.at[pl.ds(i * step, step)], zsem.at[1]).start()
        return carry
    lax.fori_loop(0, tiles_n // step, start, 0)

    per = LANES // pool
    first = lax.axis_index('table') * n_local
    lane = lax.broadcasted_iota(jnp.int32, (1, LANES), 1)
    table_n = ids_ref.shape[1]
    blocks, n_near = blocks_of(table_n)
    near = n_near * pool
    chunks = []
    for c in range(n // LANES):
        out = None
        for j in range(per):
            piece = ids_ref[blocks[c * per + j]]
            if j:
                piece = pltpu.roll(piece, j * pool, 1)
                out = jnp.where(lane >= j * pool, piece, out)
            else:
                out = piece
        chunks.append(out - first)
    ids_i = jnp.concatenate(chunks, axis=1)
    row = ids_i.astype(F32)
    tile = lax.shift_right_logical(ids_i, 3).astype(F32)
    line = jnp.bitwise_and(ids_i, 7).astype(F32)
    row_col = spread(row)
    tile_col = spread(tile)
    k_row = lax.broadcasted_iota(jnp.int32, (1, n), 1).astype(F32)
    k_col = lax.broadcasted_iota(jnp.int32, (LANES, LANES), 0).astype(F32)

    def over(fn, wide=n):
        outs = []
        for c in range(wide // LANES):
            acc = jnp.zeros((8, LANES), F32)
            for b in range(n // LANES):
                acc = acc + fn(b, c).reshape(LANES // 8, 8, LANES).sum(0)
            outs.append(acc.sum(0, keepdims=True))
        return jnp.concatenate(outs, axis=1)

    def down(val, b):
        return val[b * LANES:(b + 1) * LANES, :]

    def side(val, c):
        return val[:, c * LANES:(c + 1) * LANES]

    def ranked(val, col):
        earlier = over(lambda b, c: jnp.where((down(col, b) == side(val, c)) & (k_col + float(b * LANES) < side(k_row, c)), 1.0, 0.0))
        leader = earlier == 0.0
        lead_col = spread(jnp.where(leader, val, 1e9))
        return leader, over(lambda b, c: jnp.where(down(lead_col, b) < side(val, c), 1.0, 0.0))

    row_leader, rank = ranked(row, row_col)
    tile_leader, tile_rank = ranked(tile, tile_col)
    rank_col = spread(jnp.where(row_leader, rank, -1.0))
    tile_rank_col = spread(jnp.where(tile_leader, tile_rank, -1.0))
    spot_col = spread(tile_rank * 8.0 + line)
    spots = over(lambda b, c: jnp.where(down(rank_col, b) == side(k_row, c), down(spot_col, b), 0.0))
    tiles = over(lambda b, c: jnp.where(down(tile_rank_col, b) == side(k_row, c), down(tile_col, b), 0.0))
    lead_spot_col = spread(jnp.where(row_leader, tile_rank * 8.0 + line, 1e9))
    before = over(lambda b, c: jnp.where(down(lead_spot_col, b) < side(k_row, c) * 256.0, 1.0, 0.0), LANES)
    n_rows = jnp.sum(jnp.where(row_leader, 1.0, 0.0))
    n_tiles = jnp.sum(jnp.where(tile_leader, 1.0, 0.0))
    rank_ref[...] = rank
    lines = n // LANES
    lane_f = lane.astype(F32)
    for c in range(lines):
        spot_ref[c:c + 1, :] = jnp.where(side(k_row, c) < n_rows, side(spots, c), -1.0)
        list_ref[c:c + 1, :] = side(tiles, c).astype(jnp.int32)
    list_ref[lines:lines + 1, :] = jnp.where(lane == 0, n_tiles, n_rows).astype(jnp.int32)
    list_ref[lines + 1:lines + 2, :] = before.astype(jnp.int32)
    list_ref[lines + 2:, :] = jnp.zeros((list_ref.shape[0] - lines - 2, LANES), jnp.int32)

    flat = (table_n * pool, width)
    y_ref[...] = exact_dot(w_ref[...].T, rows_ref[:, 1].reshape(flat)).astype(BF16)
    dx_ref[...] = exact_dot(c_ref[...].T, rows_ref[:, 0].reshape(flat)).astype(BF16)

    target = lax.broadcasted_iota(jnp.int32, (LANES, near), 0).astype(F32)
    n_chunks = lax.div(n_rows.astype(jnp.int32) + (LANES - 1), LANES)

    def add_up(c, carry):
        hot = jnp.where(target + (c * LANES).astype(F32) == rank_ref[:, 0:near], 1.0, 0.0).astype(BF16)
        span = pl.ds(pl.multiple_of(c * LANES, LANES), LANES)
        for w, (out, own, prev, nxt) in enumerate(((sum_u, own_u, to_next, next_u), (sum_v, own_v, prev_v, to_prev))):
            out[span, :] = jnp.dot(hot, stack([own[...], late[w], prev[0:own.shape[0]], nxt[0:own.shape[0]]]), preferred_element_type=F32)
        return carry
    lax.fori_loop(0, n_chunks, add_up, 0)
    filled = dv_ref.at[pl.ds(0, tiles_n - REST * step)]
    pltpu.make_async_copy(du_ref, du_ref, zsem.at[0]).wait()
    pltpu.make_async_copy(filled, filled, zsem.at[1]).wait()


def fill(ids, w_all, c_all, rows, near, tiles_n, pool):
    table_n = ids.shape[1]
    n = ids.shape[0] * table_n * pool
    entries, toks = w_all.shape
    width = rows.shape[3]
    vm = pl.BlockSpec(memory_space=pltpu.VMEM)
    hbm = pl.BlockSpec(memory_space=pl.ANY)
    step = FILL
    tok_shape = jax.ShapeDtypeStruct((toks, width), BF16)
    return pl.pallas_call(
        functools.partial(fill_kernel, pool, tiles_n * 8),
        out_shape=(jax.ShapeDtypeStruct((tiles_n, 8, width), BF16),) * 2 + (tok_shape, tok_shape)
        + (jax.ShapeDtypeStruct((n, width), F32),) * 2
        + (jax.ShapeDtypeStruct((1, n), F32), jax.ShapeDtypeStruct((n // LANES, LANES), F32), jax.ShapeDtypeStruct((n // LANES + 8, LANES), jnp.int32)),
        in_specs=[vm] * 11,
        out_specs=(hbm, hbm) + (vm,) * 7,
        scratch_shapes=[
            pltpu.VMEM((step, 8, width), BF16),
            pltpu.SemaphoreType.DMA((2,)),
        ],
        compiler_params=pltpu.CompilerParams(vmem_limit_bytes=24 * MIB),
        cost_estimate=pl.CostEstimate(flops=0, bytes_accessed=2 * tiles_n * 8 * width * 2, transcendentals=0),
        name="zero_tables",
    )(ids, w_all, c_all, rows, *near)


def tiles_kernel(near, list_ref, rank_ref, spot_ref, from_prev, from_next, late_far, sum_u, sum_v, zero_u, zero_v, du_ref, dv_ref, done, stage, zero, wsem, zsem):
    n = rank_ref.shape[1]
    width = du_ref.shape[2]
    lines = n // LANES
    n_tiles = list_ref[lines, 0]
    n_rows = list_ref[lines, 1]
    n_chunks = lax.div(n_rows + (LANES - 1), LANES)
    step = zero.shape[0]
    left = FILL * REST
    kept = du_ref.shape[0] - left
    zero[...] = jnp.zeros_like(zero)

    def start(i, carry):
        pltpu.make_async_copy(zero, dv_ref.at[pl.ds(kept + i * step, step)], zsem).start()
        return carry
    lax.fori_loop(0, left // step, start, 0)

    target = lax.broadcasted_iota(jnp.int32, (LANES, n - near), 0).astype(F32)

    def finish(c, carry):
        span = pl.ds(pl.multiple_of(c * LANES, LANES), LANES)
        hot = jnp.where(target + (c * LANES).astype(F32) == rank_ref[:, near:], 1.0, 0.0).astype(BF16)
        late_n = late_far.shape[1]
        early = from_prev.shape[0] - 2 * late_n
        for w, (far, sums) in enumerate(((from_prev, sum_u), (from_next, sum_v))):
            late = [ref[early + w * late_n:early + (w + 1) * late_n] for ref in (from_prev, from_next)]
            last = jnp.dot(hot, stack(late + [late_far[w], far[0:early]]), preferred_element_type=F32)
            done[w, span, :] = (sums[span, :] + last).astype(BF16)
        return carry
    lax.fori_loop(0, n_chunks, finish, 0)

    tall = 256
    per = tall // 8
    place = lax.broadcasted_iota(jnp.int32, (tall, LANES), 0).astype(F32)

    ring = stage.shape[0]
    n_builds = lax.div(n_tiles + per - 1, per)

    def drain(slot):
        pltpu.make_async_copy(stage.at[slot], stage.at[slot], wsem.at[slot]).wait()

    def build(c, carry):
        slot = lax.rem(c, ring)
        start = lax.div(list_ref[lines + 1, c], LANES)
        end = lax.div(list_ref[lines + 1, c + 1] + (LANES - 1), LANES)

        def lay(kc):
            hot = jnp.where(place + (c * tall).astype(F32) == spot_ref[pl.ds(kc, 1), :], 1.0, 0.0).astype(BF16)
            span = pl.ds(pl.multiple_of(kc * LANES, LANES), LANES)
            return [jnp.dot(hot, done[w, span, :], preferred_element_type=F32).astype(BF16).reshape(per, 8, width) for w in range(2)]
        for w, val in enumerate(lay(start)):
            stage[slot, w] = val

        def more(kc, inner):
            for w, val in enumerate(lay(kc)):
                stage[slot, w] = stage[slot, w] + val
            return inner
        lax.fori_loop(start + 1, end, more, 0)
        return carry

    def put(c, w, ref):
        slot = lax.rem(c, ring)
        line = lax.div(c * per, LANES)
        base = lax.rem(c * per, LANES)
        count = n_tiles - c * per

        def one(i, carry):
            pltpu.make_async_copy(stage.at[slot, w, i], ref.at[list_ref[line, base + i]], wsem.at[slot]).start()
            return carry

        @pl.when(count >= per)
        def _():
            for i in range(per):
                one(i, 0)

        @pl.when(count < per)
        def _():
            lax.fori_loop(0, count, one, 0)

    def first(c, carry):
        build(c, 0)
        put(c, 0, du_ref)
        return carry
    lax.fori_loop(0, jnp.minimum(n_builds, ring), first, 0)
    tail = dv_ref.at[pl.ds(kept, left)]
    pltpu.make_async_copy(tail, tail, zsem).wait()

    def second(c, carry):
        put(c, 1, dv_ref)
        return carry
    lax.fori_loop(0, jnp.minimum(n_builds, ring), second, 0)

    def later(c, carry):
        drain(lax.rem(c, ring))
        build(c, 0)
        put(c, 0, du_ref)
        put(c, 1, dv_ref)
        return carry
    lax.fori_loop(ring, n_builds, later, 0)

    def full(c, carry):
        drain(lax.rem(c, ring))
        return carry
    lax.fori_loop(jnp.maximum(0, n_builds - ring), n_builds - 1, full, 0)
    slot = lax.rem(n_builds - 1, ring)

    def rest(q, carry):
        for w, ref in enumerate((du_ref, dv_ref)):
            pltpu.make_async_copy(stage.at[slot, w, 0], ref.at[0], wsem.at[slot]).wait()
        return carry
    lax.fori_loop((n_builds - 1) * per, n_tiles, rest, 0)


def write_tiles(lst, rank, spot, far, sum_u, sum_v, zero_u, zero_v, near):
    n = rank.shape[1]
    tiles_n, _, width = zero_u.shape
    vm = pl.BlockSpec(memory_space=pltpu.VMEM)
    hbm = pl.BlockSpec(memory_space=pl.ANY)
    return pl.pallas_call(
        functools.partial(tiles_kernel, near),
        out_shape=(jax.ShapeDtypeStruct((tiles_n, 8, width), BF16),) * 2,
        in_specs=[pl.BlockSpec(memory_space=pltpu.SMEM)] + [vm] * 7 + [hbm] * 2,
        out_specs=(hbm, hbm),
        scratch_shapes=[
            pltpu.VMEM((2, n, width), BF16),
            pltpu.VMEM((8, 2, 32, 8, width), BF16),
            pltpu.VMEM((FILL // 2, 8, width), BF16),
            pltpu.SemaphoreType.DMA((8,)),
            pltpu.SemaphoreType.DMA,
        ],
        input_output_aliases={8: 0, 9: 1},
        compiler_params=pltpu.CompilerParams(vmem_limit_bytes=24 * MIB),
        name="write_tiles",
    )(lst, rank, spot, *far, sum_u, sum_v, zero_u, zero_v)


def solution(mesh):
    table_n = mesh.shape['table']
    data_n = mesh.shape['data']
    tok_spec = P(('replica', 'data', 'table'))
    row_spec = P(('replica', 'table'))
    up = [(i, (i + 1) % data_n) for i in range(data_n)]
    down = [(i, (i + data_n - 1) % data_n) for i in range(data_n)]
    over = [(i, (i + 2) % data_n) for i in range(data_n)]

    def device_step(tok_loc, dy_loc, u_loc, v_loc, wanted_loc, pick_loc, gate_loc):
        n_local, width = u_loc.shape
        toks = tok_loc.shape[0]
        pool = wanted_loc.shape[1] // table_n
        tiles_n = n_local // 8
        pick = pick_loc.transpose(1, 2, 0).reshape(-1, toks)
        gate = gate_loc.transpose(1, 2, 0).reshape(-1, toks)
        ids = share_ids(wanted_loc, table_n, pool)
        rows = fetch(ids, u_loc.reshape(tiles_n, 8, width), v_loc.reshape(tiles_n, 8, width), table_n, pool)
        w_all, c_all, rows_in, own_u, own_v, to_next, prev_v, next_u, to_prev, late, all_ids = exchange(rows, tok_loc, dy_loc, pick, gate, ids, table_n, data_n, pool)
        far = (lax.ppermute(to_next, 'data', up), lax.ppermute(to_prev, 'data', down), lax.ppermute(late, 'data', over))
        near = (own_u, own_v, to_next, prev_v, next_u, to_prev, late)
        zero_u, zero_v, y_loc, dx_loc, sum_u, sum_v, rank, spot, lst = fill(all_ids, w_all, c_all, rows_in, near, tiles_n, pool)
        grad_u, grad_v = write_tiles(lst, rank, spot, far, sum_u, sum_v, zero_u, zero_v, blocks_of(table_n)[1] * pool)
        return y_loc, dx_loc, grad_u.reshape(n_local, width), grad_v.reshape(n_local, width)

    return jax.shard_map(device_step, mesh=mesh, in_specs=(tok_spec, tok_spec, row_spec, row_spec, tok_spec, tok_spec, tok_spec), out_specs=(tok_spec, tok_spec, row_spec, row_spec), check_vma=False)
```
